32 devices in a mesh: data: 32 (over z, y, x, core).
Axes of the slice: x: 2, y: 2, z: 4, core: 2. Of those that a mesh axis runs over, the one named last changes fastest.
Arguments:
- h_a: bfloat16 [16384, 384], P('data')
- h_b: bfloat16 [16384, 384], P('data')
- w_one: bfloat16 [384, 2048], replicated
- w_two: bfloat16 [2048, 2048], replicated
- w_three: bfloat16 [2048, 2048], replicated
- gain_one: float32 [2048], replicated
- shift_one: float32 [2048], replicated
- gain_two: float32 [2048], replicated
- shift_two: float32 [2048], replicated
- lam_off: float32 [], replicated
Outputs:
- output 1: float32 [], replicated
- output 2: float32 [384, 2048], P('data')
- output 3: float32 [2048, 2048], P('data')
- output 4: float32 [2048, 2048], P('data')
- output 5: float32 [2048], replicated
- output 6: float32 [2048], replicated
- output 7: float32 [2048], replicated
- output 8: float32 [2048], replicated
All inputs are finite; a program needn't handle non-finite values.
Results may differ from the reference program's by a relative error of at most 0.00504156.
Values are sent between devices in bfloat16 or wider.
A program may use at most 1 GiB of HBM per device.

```python
import jax
import jax.numpy as jnp
from jax import lax

FEAT_DIM = 384
PROJ_DIM = 2048
ROWS_DEV = 512
SHARDS = 32
TOTAL_ROWS = ROWS_DEV * SHARDS
NORM_EPS = 1e-5


def setup_inputs(seed: int = 0) -> dict:
    key_list = jax.random.split(jax.random.key(seed), 14)
    common = jax.random.normal(key_list[0], (TOTAL_ROWS, FEAT_DIM), jnp.float32)
    shard_shift = 0.6 * jax.random.normal(key_list[1], (SHARDS, 1, FEAT_DIM), jnp.float32)
    shard_scale = jnp.exp(0.3 * jax.random.normal(key_list[2], (SHARDS, 1, FEAT_DIM), jnp.float32))

    def make_view(view_key):
        noise_vals = jax.random.normal(view_key, (TOTAL_ROWS, FEAT_DIM), jnp.float32)
        mixed_rows = (0.77 * common + 0.64 * noise_vals).reshape(SHARDS, ROWS_DEV, FEAT_DIM)
        return (mixed_rows * shard_scale + shard_shift).reshape(TOTAL_ROWS, FEAT_DIM).astype(jnp.bfloat16)

    def make_weight(weight_key, fan_in, fan_out):
        weight_scale = fan_in ** -0.5
        return (jax.random.normal(weight_key, (fan_in, fan_out), jnp.float32) * weight_scale).astype(jnp.bfloat16)

    def make_vector(vec_key, center):
        return center + 0.25 * jax.random.normal(vec_key, (PROJ_DIM,), jnp.float32)

    lam_off = (0.1 + 0.2 * jax.random.uniform(key_list[12], (), jnp.float32)) * TOTAL_ROWS / PROJ_DIM
    return {
        "h_a": make_view(key_list[3]),
        "h_b": make_view(key_list[4]),
        "w_one": make_weight(key_list[5], FEAT_DIM, PROJ_DIM),
        "w_two": make_weight(key_list[6], PROJ_DIM, PROJ_DIM),
        "w_three": make_weight(key_list[7], PROJ_DIM, PROJ_DIM),
        "gain_one": make_vector(key_list[8], 1.0),
        "shift_one": make_vector(key_list[9], 0.0),
        "gain_two": make_vector(key_list[10], 1.0),
        "shift_two": make_vector(key_list[11], 0.0),
        "lam_off": lam_off,
    }


def batch_norm(values):
    col_mean = jnp.sum(values, axis=0) / TOTAL_ROWS
    col_var = jnp.sum(values * values, axis=0) / TOTAL_ROWS - col_mean * col_mean
    return (values - col_mean) * lax.rsqrt(col_var + NORM_EPS)


def project(feat_rows, params):
    w_one, w_two, w_three, gain_one, shift_one, gain_two, shift_two = params
    hidden_one = jnp.dot(feat_rows.astype(jnp.float32), w_one, preferred_element_type=jnp.float32)
    act_one = jax.nn.relu(gain_one * batch_norm(hidden_one) + shift_one).astype(jnp.bfloat16)
    hidden_two = jnp.dot(act_one.astype(jnp.float32), w_two, preferred_element_type=jnp.float32)
    act_two = jax.nn.relu(gain_two * batch_norm(hidden_two) + shift_two).astype(jnp.bfloat16)
    proj_out = jnp.dot(act_two.astype(jnp.float32), w_three, preferred_element_type=jnp.float32)
    return batch_norm(proj_out).astype(jnp.bfloat16)


def barlow_loss(params, h_a, h_b, lam_off):
    embed_a = project(h_a, params).astype(jnp.float32)
    embed_b = project(h_b, params).astype(jnp.float32)
    corr_mat = jnp.dot(embed_a.T, embed_b, preferred_element_type=jnp.float32) / TOTAL_ROWS
    feat_index = jnp.arange(PROJ_DIM)
    diag_mask = feat_index[:, None] == feat_index[None, :]
    diag_gap = 1.0 - jnp.diagonal(corr_mat)
    off_square = jnp.sum(jnp.where(diag_mask, 0.0, corr_mat * corr_mat))
    return jnp.sum(diag_gap * diag_gap) + lam_off * off_square


def reference(h_a, h_b, w_one, w_two, w_three, gain_one, shift_one, gain_two, shift_two, lam_off):
    params = (w_one.astype(jnp.float32), w_two.astype(jnp.float32), w_three.astype(jnp.float32),
              gain_one, shift_one, gain_two, shift_two)
    loss_total, grad_list = jax.value_and_grad(barlow_loss)(params, h_a, h_b, lam_off)
    return (loss_total, grad_list[0], grad_list[1], grad_list[2],
            grad_list[3], grad_list[4], grad_list[5], grad_list[6])
```

```python
import functools

import jax
import jax.numpy as jnp
from jax import lax
from jax.experimental import pallas as pl
from jax.experimental.pallas import tpu as pltpu
from jax.sharding import PartitionSpec as P

NORM_EPS = 1e-5
FIRST_DIMS = (((0,), (0,)), ((), ()))
LAST_DIMS = (((2,), (1,)), ((), ()))
MESH = pl.DeviceIdType.MESH
VMEM = pl.BlockSpec(memory_space=pltpu.VMEM)
AXIS = "data"
CHUNK = 256
HALF = 128
LIMIT = 60 * 1024 * 1024


def coords():
    me = lax.axis_index(AXIS)
    return me, me // 8, (me // 4) % 2, (me // 2) % 2, me % 2


def device_of(z, y, x, c):
    return ((z * 2 + y) * 2 + x) * 2 + c


def greet(peers):
    barrier = pltpu.get_barrier_semaphore()
    for peer in peers:
        pl.semaphore_signal(barrier, inc=1, device_id=(peer,), device_id_type=MESH)
    pl.semaphore_wait(barrier, len(peers))


def remote(src, dst, send_sem, recv_sem, peer):
    return pltpu.make_async_remote_copy(src_ref=src, dst_ref=dst, send_sem=send_sem, recv_sem=recv_sem,
                                        device_id=(peer,), device_id_type=MESH)


def params(collective_id):
    return pltpu.CompilerParams(collective_id=collective_id, has_side_effects=True, vmem_limit_bytes=LIMIT)


def sums_kernel(part_ref, out_ref, in_plane, own, in_line, total,
                send_a, recv_a, send_b, recv_b, send_c, recv_c):
    me = lax.axis_index(AXIS)
    z, q = me // 8, me % 8
    width = part_ref.shape[1] // 8

    def cols(k):
        return pl.ds(pl.multiple_of(k * width, width), width)

    plane = [(q + d) % 8 for d in range(1, 8)]
    line = [(z + d) % 4 for d in range(1, 4)]
    greet([z * 8 + p for p in plane] + [p * 8 + q for p in line])
    first = [remote(part_ref.at[:, cols(p)], in_plane.at[d], send_a.at[d], recv_a.at[d], z * 8 + p)
             for d, p in enumerate(plane)]
    for copy in first:
        copy.start()
    acc = part_ref[:, cols(q)]
    for d, copy in enumerate(first):
        copy.wait()
        acc = acc + in_plane[d]
    own[...] = acc
    in_line[z] = acc
    second = [remote(own, in_line.at[z], send_b.at[d], recv_b.at[d], p * 8 + q) for d, p in enumerate(line)]
    for copy in second:
        copy.start()
    for copy in second:
        copy.wait()
    acc = (in_line[0] + in_line[1]) + (in_line[2] + in_line[3])
    total[...] = acc
    out_ref[:, cols(q)] = acc
    third = [remote(total, out_ref.at[:, cols(q)], send_c.at[d], recv_c.at[d], z * 8 + p)
             for d, p in enumerate(plane)]
    for copy in third:
        copy.start()
    for copy in third:
        copy.wait()


def all_sums(part, collective_id):
    rows, features = part.shape
    width = features // 8
    dma = pltpu.SemaphoreType.DMA
    return pl.pallas_call(
        sums_kernel,
        out_shape=jax.ShapeDtypeStruct((rows, features), jnp.float32),
        in_specs=[VMEM], out_specs=VMEM,
        scratch_shapes=[pltpu.VMEM((7, rows, width), jnp.float32), pltpu.VMEM((rows, width), jnp.float32),
                        pltpu.VMEM((4, rows, width), jnp.float32), pltpu.VMEM((rows, width), jnp.float32),
                        dma((7,)), dma((7,)), dma((3,)), dma((3,)), dma((7,)), dma((7,))],
        compiler_params=params(collective_id),
        name="all_sums",
    )(part)


def scatter_kernel(CHUNK, turned, lhs_ref, rhs_ref, out_ref, part, in_core, in_one_a, in_one_b, in_two_a, in_two_b, in_line,
                   sc, rc, s1a, r1a, s1b, r1b, s2a, r2a, s2b, r2b, s3, r3):
    me, z, y, x, c = coords()
    core_peer = device_of(z, y, x, 1 - c)
    x_peer = device_of(z, y, 1 - x, c)
    y_peer = device_of(z, 1 - y, x, c)
    line = [(z + d) % 4 for d in range(1, 4)]
    line_peers = [device_of(p, y, x, c) for p in line]
    chunks = rhs_ref.shape[1] // CHUNK
    rows = out_ref.shape[0]
    quarter = 8 * rows
    HALF = CHUNK // 2
    greet([core_peer, x_peer, y_peer] + line_peers)

    def both(j):
        return pl.ds(pl.multiple_of(j * CHUNK, CHUNK), CHUNK)

    def half_a(j):
        return pl.ds(pl.multiple_of(j * CHUNK, HALF), HALF)

    def half_b(j):
        return pl.ds(pl.multiple_of(j * CHUNK + HALF, HALF), HALF)

    def packed(j):
        return pl.ds(pl.multiple_of(j * HALF, HALF), HALF)

    def core_copy(j):
        return remote(part.at[:, :, :, 1 - c, :, both(j)], in_core.at[:, :, :, :, both(j)],
                      sc.at[j], rc.at[j], core_peer)

    def one_copies(j):
        return (remote(part.at[:, :, 1 - x, c, :, half_a(j)], in_one_a.at[:, :, :, packed(j)],
                       s1a.at[j], r1a.at[j], x_peer),
                remote(part.at[:, 1 - y, :, c, :, half_b(j)], in_one_b.at[:, :, :, packed(j)],
                       s1b.at[j], r1b.at[j], y_peer))

    def two_copies(j):
        return (remote(part.at[:, 1 - y, x, c, :, half_a(j)], in_two_a.at[:, :, packed(j)],
                       s2a.at[j], r2a.at[j], y_peer),
                remote(part.at[:, y, 1 - x, c, :, half_b(j)], in_two_b.at[:, :, packed(j)],
                       s2b.at[j], r2b.at[j], x_peer))

    def line_copies(j):
        return [remote(part.at[p, y, x, c, :, both(j)], in_line.at[d, :, both(j)],
                       s3.at[d, j], r3.at[d, j], line_peers[d]) for d, p in enumerate(line)]

    def step(t, carry):
        @pl.when(jnp.logical_and(t >= 4, t < chunks + 4))
        def _():
            j = t - 4
            copies = line_copies(j)
            for copy in copies:
                copy.wait()
            out_ref[:, both(j)] = ((part[z, y, x, c, :, both(j)] + in_line[0, :, both(j)])
                                   + (in_line[1, :, both(j)] + in_line[2, :, both(j)]))

        @pl.when(jnp.logical_and(t >= 3, t < chunks + 3))
        def _():
            j = t - 3
            for copy in two_copies(j):
                copy.wait()
            for w in range(4):
                part[w, y, x, c, :, half_a(j)] += in_two_a[w, :, packed(j)]
                part[w, y, x, c, :, half_b(j)] += in_two_b[w, :, packed(j)]
            for copy in line_copies(j):
                copy.start()

        @pl.when(jnp.logical_and(t >= 2, t < chunks + 2))
        def _():
            j = t - 2
            for copy in one_copies(j):
                copy.wait()
            for w in range(4):
                for v in range(2):
                    part[w, v, x, c, :, half_a(j)] += in_one_a[w, v, :, packed(j)]
                    part[w, y, v, c, :, half_b(j)] += in_one_b[w, v, :, packed(j)]
            for copy in two_copies(j):
                copy.start()

        @pl.when(jnp.logical_and(t >= 1, t < chunks + 1))
        def _():
            j = t - 1
            core_copy(j).wait()
            for w in range(4):
                for v in range(2):
                    for u in range(2):
                        part[w, v, u, c, :, both(j)] += in_core[w, v, u, :, both(j)]
            for copy in one_copies(j):
                copy.start()

        @pl.when(t < chunks)
        def _():
            rhs = rhs_ref[:, both(t)]

            def tile(w, carry):
                span = pl.ds(pl.multiple_of(w * quarter, quarter), quarter)
                if turned:
                    product = jnp.dot(lhs_ref[span, :], rhs, preferred_element_type=jnp.float32)
                else:
                    product = lax.dot_general(lhs_ref[:, span], rhs, FIRST_DIMS, preferred_element_type=jnp.float32)
                part[w, :, :, :, :, both(t)] = product.reshape(2, 2, 2, rows, CHUNK)
                return carry

            lax.fori_loop(0, 4, tile, 0)
            core_copy(t).start()

        return carry

    lax.fori_loop(0, chunks + 4, step, 0)


def product_scatter(lhs, rhs, collective_id, chunk=CHUNK, turned=False):
    total, depth = lhs.shape if turned else lhs.shape[::-1]
    features = rhs.shape[1]
    rows = total // 32
    chunks = features // chunk
    dma = pltpu.SemaphoreType.DMA
    f32 = jnp.float32
    return pl.pallas_call(
        functools.partial(scatter_kernel, chunk, turned),
        out_shape=jax.ShapeDtypeStruct((rows, features), f32),
        in_specs=[VMEM, VMEM], out_specs=VMEM,
        scratch_shapes=[pltpu.VMEM((4, 2, 2, 2, rows, features), f32), pltpu.VMEM((4, 2, 2, rows, features), f32),
                        pltpu.VMEM((4, 2, rows, features // 2), f32), pltpu.VMEM((4, 2, rows, features // 2), f32),
                        pltpu.VMEM((4, rows, features // 2), f32), pltpu.VMEM((4, rows, features // 2), f32),
                        pltpu.VMEM((3, rows, features), f32)]
                       + [dma((chunks,))] * 10 + [dma((3, chunks))] * 2,
        compiler_params=params(collective_id),
        cost_estimate=pl.CostEstimate(flops=2 * total * depth * features, bytes_accessed=4 * total * features,
                                      transcendentals=0),
        name="product_scatter",
    )(lhs, rhs)


def gather_kernel(block_ref, a_ref, b_ref, grad_a_ref, grad_b_ref, whole,
                  s3, r3, s2a, r2a, s2b, r2b, s1a, r1a, s1b, r1b, sc, rc):
    me, z, y, x, c = coords()
    core_peer = device_of(z, y, x, 1 - c)
    x_peer = device_of(z, y, 1 - x, c)
    y_peer = device_of(z, 1 - y, x, c)
    line = [(z + d) % 4 for d in range(1, 4)]
    line_peers = [device_of(p, y, x, c) for p in line]
    rows, features = block_ref.shape
    chunks = features // CHUNK
    greet([core_peer, x_peer, y_peer] + line_peers)

    def both(j):
        return pl.ds(pl.multiple_of(j * CHUNK, CHUNK), CHUNK)

    def half_a(j):
        return pl.ds(pl.multiple_of(j * CHUNK, HALF), HALF)

    def half_b(j):
        return pl.ds(pl.multiple_of(j * CHUNK + HALF, HALF), HALF)

    def line_copies(j):
        return [remote(block_ref.at[:, both(j)], whole.at[z, y, x, c, :, both(j)],
                       s3.at[d, j], r3.at[d, j], line_peers[d]) for d in range(3)]

    def two_copies(j):
        a, b = whole.at[:, y, x, c, :, half_a(j)], whole.at[:, y, x, c, :, half_b(j)]
        return (remote(a, a, s2a.at[j], r2a.at[j], y_peer), remote(b, b, s2b.at[j], r2b.at[j], x_peer))

    def one_copies(j):
        a, b = whole.at[:, :, x, c, :, half_a(j)], whole.at[:, y, :, c, :, half_b(j)]
        return (remote(a, a, s1a.at[j], r1a.at[j], x_peer), remote(b, b, s1b.at[j], r1b.at[j], y_peer))

    def core_copy(j):
        a = whole.at[:, :, :, c, :, both(j)]
        return remote(a, a, sc.at[j], rc.at[j], core_peer)

    whole[z, y, x, c] = block_ref[...]
    grad_a_ref[...] = jnp.zeros_like(grad_a_ref)

    def step(t, carry):
        @pl.when(t < chunks)
        def _():
            for copy in line_copies(t):
                copy.start()

        @pl.when(jnp.logical_and(t >= 1, t < chunks + 1))
        def _():
            for copy in line_copies(t - 1):
                copy.wait()
            for copy in two_copies(t - 1):
                copy.start()

        @pl.when(jnp.logical_and(t >= 2, t < chunks + 2))
        def _():
            for copy in two_copies(t - 2):
                copy.wait()
            for copy in one_copies(t - 2):
                copy.start()

        @pl.when(jnp.logical_and(t >= 3, t < chunks + 3))
        def _():
            for copy in one_copies(t - 3):
                copy.wait()
            core_copy(t - 3).start()

        @pl.when(t >= 4)
        def _():
            j = t - 4
            core_copy(j).wait()
            slab = whole[:, :, :, :, :, both(j)].reshape(32 * rows, CHUNK)
            grad_b_ref[:, both(j)] = jnp.dot(a_ref[...], slab, preferred_element_type=jnp.float32)
            grad_a_ref[...] += lax.dot_general(b_ref[:, both(j)], slab, (((1,), (1,)), ((), ())),
                                               preferred_element_type=jnp.float32)

        return carry

    lax.fori_loop(0, chunks + 4, step, 0)


def gather_products(block, embed_a, embed_b, collective_id):
    rows, features = block.shape
    chunks = features // CHUNK
    dma = pltpu.SemaphoreType.DMA
    shape = jax.ShapeDtypeStruct(embed_a.shape, jnp.float32)
    return pl.pallas_call(
        gather_kernel,
        out_shape=(shape, shape),
        in_specs=[VMEM] * 3, out_specs=(VMEM, VMEM),
        scratch_shapes=[pltpu.VMEM((4, 2, 2, 2, rows, features), jnp.bfloat16)]
                       + [dma((3, chunks))] * 2 + [dma((chunks,))] * 10,
        compiler_params=params(collective_id),
        cost_estimate=pl.CostEstimate(flops=4 * embed_a.size * features, bytes_accessed=4 * features * features,
                                      transcendentals=0),
        name="gather_products",
    )(block, embed_a, embed_b)


def norm_forward(values, total_rows, collective_id):
    part = jnp.concatenate([jnp.sum(values, axis=1), jnp.sum(values * values, axis=1)])
    col_sums = all_sums(part, collective_id).reshape(2, 2, -1)
    col_mean = col_sums[0] / total_rows
    inv_std = lax.rsqrt(col_sums[1] / total_rows - col_mean * col_mean + NORM_EPS)
    return (values - col_mean[:, None, :]) * inv_std[:, None, :], inv_std


def norm_backward(grad_out, normed, inv_std, total_rows, collective_id, extra=None):
    rows = [jnp.sum(grad_out, axis=1), jnp.sum(grad_out * normed, axis=1)]
    sums = all_sums(jnp.concatenate(rows if extra is None else rows + [extra]), collective_id)
    col_sums = sums[:4].reshape(2, 2, -1)
    grad_in = inv_std[:, None, :] * (grad_out - (col_sums[0][:, None, :] + normed * col_sums[1][:, None, :]) / total_rows)
    return grad_in, col_sums, sums[4:]


def solution(mesh):
    shards = mesh.shape[AXIS]

    def local_step(h_a, h_b, w_one, w_two, w_three, gain_one, shift_one, gain_two, shift_two, lam_off):
        me = lax.axis_index(AXIS)
        rows_dev = h_a.shape[0]
        total_rows = rows_dev * shards
        features = w_two.shape[0]
        feat_rows = jnp.concatenate([h_a, h_b], axis=0)
        in_rows = feat_rows.shape[1] // shards
        feat_t = jnp.pad(feat_rows.T.reshape(shards, in_rows, 2 * rows_dev), ((0, 0), (0, 16 - in_rows), (0, 0)))
        feat_t = feat_t.reshape(shards * 16, 2 * rows_dev)
        hidden_one = jnp.dot(feat_rows, w_one, preferred_element_type=jnp.float32).reshape(2, rows_dev, -1)
        normed_one, inv_one = norm_forward(hidden_one, total_rows, 0)
        pre_one = gain_one * normed_one + shift_one
        act_one = jax.nn.relu(pre_one).astype(jnp.bfloat16)
        hidden_two = jnp.dot(act_one, w_two, preferred_element_type=jnp.float32)
        normed_two, inv_two = norm_forward(hidden_two, total_rows, 1)
        pre_two = gain_two * normed_two + shift_two
        act_two = jax.nn.relu(pre_two).astype(jnp.bfloat16)
        proj_out = jnp.dot(act_two, w_three, preferred_element_type=jnp.float32)
        normed_out, inv_out = norm_forward(proj_out, total_rows, 2)
        embed_pair = normed_out.astype(jnp.bfloat16)
        corr_rows = product_scatter(embed_pair[0], embed_pair[1], 3) / total_rows
        block_rows = features // shards
        row_index = me * block_rows + jnp.arange(block_rows)
        diag_mask = row_index[:, None] == jnp.arange(features)[None, :]
        diag_gap = 1.0 - corr_rows
        loss_part = jnp.sum(jnp.where(diag_mask, diag_gap * diag_gap, lam_off * corr_rows * corr_rows),
                            axis=0, keepdims=True)
        grad_corr = jnp.where(diag_mask, -2.0 * diag_gap, 2.0 * lam_off * corr_rows)
        grad_scaled = (grad_corr / total_rows).astype(jnp.bfloat16)
        grad_embed = jnp.stack(gather_products(grad_scaled, embed_pair[0], embed_pair[1], 4))
        grad_proj, _, loss_row = norm_backward(grad_embed, normed_out, inv_out, total_rows, 5, loss_part)
        grad_proj = grad_proj.astype(jnp.bfloat16)
        loss_total = jnp.sum(loss_row)

        def flat(value):
            return value.reshape(2 * rows_dev, -1)

        grad_w_three = product_scatter(flat(act_two), flat(grad_proj), 6)
        grad_act_two = lax.dot_general(grad_proj, w_three, LAST_DIMS, preferred_element_type=jnp.float32)
        grad_pre_two = jnp.where(pre_two > 0, grad_act_two, 0.0)
        grad_hidden_two, sums_two, _ = norm_backward(grad_pre_two, normed_two, inv_two, total_rows, 7)
        grad_hidden_two = (gain_two * grad_hidden_two).astype(jnp.bfloat16)
        grad_w_two = product_scatter(flat(act_one), flat(grad_hidden_two), 8)
        grad_act_one = lax.dot_general(grad_hidden_two, w_two, LAST_DIMS, preferred_element_type=jnp.float32)
        grad_pre_one = jnp.where(pre_one > 0, grad_act_one, 0.0)
        grad_hidden_one, sums_one, _ = norm_backward(grad_pre_one, normed_one, inv_one, total_rows, 9)
        grad_hidden_one = (gain_one * grad_hidden_one).astype(jnp.bfloat16)
        grad_w_one = product_scatter(feat_t, flat(grad_hidden_one), 10, 512, True)[:in_rows]
        return (loss_total, grad_w_one, grad_w_two, grad_w_three,
                jnp.sum(sums_one[1], axis=0), jnp.sum(sums_one[0], axis=0),
                jnp.sum(sums_two[1], axis=0), jnp.sum(sums_two[0], axis=0))

    row_spec = P(AXIS, None)
    whole_mat = P(None, None)
    whole_vec = P(None)
    return jax.shard_map(
        local_step, mesh=mesh,
        in_specs=(row_spec, row_spec, whole_mat, whole_mat, whole_mat,
                  whole_vec, whole_vec, whole_vec, whole_vec, P()),
        out_specs=(P(), row_spec, row_spec, row_spec, whole_vec, whole_vec, whole_vec, whole_vec),
        check_vma=False)
```

```python
import functools

import jax
import jax.numpy as jnp
from jax import lax
from jax.experimental import pallas as pl
from jax.experimental.pallas import tpu as pltpu
from jax.sharding import PartitionSpec as P

NORM_EPS = 1e-5
FIRST_DIMS = (((0,), (0,)), ((), ()))
MESH = pl.DeviceIdType.MESH
VMEM = pl.BlockSpec(memory_space=pltpu.VMEM)
AXIS = "data"
CHUNK = 256
HALF = 128
LIMIT = 60 * 1024 * 1024


def coords():
    me = lax.axis_index(AXIS)
    return me, me // 8, (me // 4) % 2, (me // 2) % 2, me % 2


def device_of(z, y, x, c):
    return ((z * 2 + y) * 2 + x) * 2 + c


def greet(peers):
    barrier = pltpu.get_barrier_semaphore()
    for peer in peers:
        pl.semaphore_signal(barrier, inc=1, device_id=(peer,), device_id_type=MESH)
    pl.semaphore_wait(barrier, len(peers))


def remote(src, dst, send_sem, recv_sem, peer):
    return pltpu.make_async_remote_copy(src_ref=src, dst_ref=dst, send_sem=send_sem, recv_sem=recv_sem,
                                        device_id=(peer,), device_id_type=MESH)


def params(collective_id):
    return pltpu.CompilerParams(collective_id=collective_id, has_side_effects=True, vmem_limit_bytes=LIMIT)


def sums_kernel(part_ref, out_ref, in_plane, own, in_line, total,
                send_a, recv_a, send_b, recv_b, send_c, recv_c):
    me = lax.axis_index(AXIS)
    z, q = me // 8, me % 8
    width = part_ref.shape[1] // 8

    def cols(k):
        return pl.ds(pl.multiple_of(k * width, width), width)

    plane = [(q + d) % 8 for d in range(1, 8)]
    line = [(z + d) % 4 for d in range(1, 4)]
    greet([z * 8 + p for p in plane] + [p * 8 + q for p in line])
    first = [remote(part_ref.at[:, cols(p)], in_plane.at[d], send_a.at[d], recv_a.at[d], z * 8 + p)
             for d, p in enumerate(plane)]
    for copy in first:
        copy.start()
    acc = part_ref[:, cols(q)]
    for d, copy in enumerate(first):
        copy.wait()
        acc = acc + in_plane[d]
    own[...] = acc
    in_line[z] = acc
    second = [remote(own, in_line.at[z], send_b.at[d], recv_b.at[d], p * 8 + q) for d, p in enumerate(line)]
    for copy in second:
        copy.start()
    for copy in second:
        copy.wait()
    acc = (in_line[0] + in_line[1]) + (in_line[2] + in_line[3])
    total[...] = acc
    out_ref[:, cols(q)] = acc
    third = [remote(total, out_ref.at[:, cols(q)], send_c.at[d], recv_c.at[d], z * 8 + p)
             for d, p in enumerate(plane)]
    for copy in third:
        copy.start()
    for copy in third:
        copy.wait()


def all_sums(part, collective_id):
    rows, features = part.shape
    width = features // 8
    dma = pltpu.SemaphoreType.DMA
    return pl.pallas_call(
        sums_kernel,
        out_shape=jax.ShapeDtypeStruct((rows, features), jnp.float32),
        in_specs=[VMEM], out_specs=VMEM,
        scratch_shapes=[pltpu.VMEM((7, rows, width), jnp.float32), pltpu.VMEM((rows, width), jnp.float32),
                        pltpu.VMEM((4, rows, width), jnp.float32), pltpu.VMEM((rows, width), jnp.float32),
                        dma((7,)), dma((7,)), dma((3,)), dma((3,)), dma((7,)), dma((7,))],
        compiler_params=params(collective_id),
        name="all_sums",
    )(part)


def scatter_kernel(CHUNK, turned, lhs_ref, rhs_ref, out_ref, part, in_core, in_one_a, in_one_b, in_two_a, in_two_b, in_line,
                   sc, rc, s1a, r1a, s1b, r1b, s2a, r2a, s2b, r2b, s3, r3):
    me, z, y, x, c = coords()
    core_peer = device_of(z, y, x, 1 - c)
    x_peer = device_of(z, y, 1 - x, c)
    y_peer = device_of(z, 1 - y, x, c)
    line = [(z + d) % 4 for d in range(1, 4)]
    line_peers = [device_of(p, y, x, c) for p in line]
    chunks = rhs_ref.shape[1] // CHUNK
    rows = out_ref.shape[0]
    quarter = 8 * rows
    HALF = CHUNK // 2
    greet([core_peer, x_peer, y_peer] + line_peers)

    def both(j):
        return pl.ds(pl.multiple_of(j * CHUNK, CHUNK), CHUNK)

    def half_a(j):
        return pl.ds(pl.multiple_of(j * CHUNK, HALF), HALF)

    def half_b(j):
        return pl.ds(pl.multiple_of(j * CHUNK + HALF, HALF), HALF)

    def packed(j):
        return pl.ds(pl.multiple_of(j * HALF, HALF), HALF)

    def core_copy(j):
        return remote(part.at[:, :, :, 1 - c, :, both(j)], in_core.at[:, :, :, :, both(j)],
                      sc.at[j], rc.at[j], core_peer)

    def one_copies(j):
        return (remote(part.at[:, :, 1 - x, c, :, half_a(j)], in_one_a.at[:, :, :, packed(j)],
                       s1a.at[j], r1a.at[j], x_peer),
                remote(part.at[:, 1 - y, :, c, :, half_b(j)], in_one_b.at[:, :, :, packed(j)],
                       s1b.at[j], r1b.at[j], y_peer))

    def two_copies(j):
        return (remote(part.at[:, 1 - y, x, c, :, half_a(j)], in_two_a.at[:, :, packed(j)],
                       s2a.at[j], r2a.at[j], y_peer),
                remote(part.at[:, y, 1 - x, c, :, half_b(j)], in_two_b.at[:, :, packed(j)],
                       s2b.at[j], r2b.at[j], x_peer))

    def line_copies(j):
        return [remote(part.at[p, y, x, c, :, both(j)], in_line.at[d, :, both(j)],
                       s3.at[d, j], r3.at[d, j], line_peers[d]) for d, p in enumerate(line)]

    def step(t, carry):
        @pl.when(jnp.logical_and(t >= 4, t < chunks + 4))
        def _():
            j = t - 4
            copies = line_copies(j)
            for copy in copies:
                copy.wait()
            out_ref[:, both(j)] = ((part[z, y, x, c, :, both(j)] + in_line[0, :, both(j)])
                                   + (in_line[1, :, both(j)] + in_line[2, :, both(j)]))

        @pl.when(jnp.logical_and(t >= 3, t < chunks + 3))
        def _():
            j = t - 3
            for copy in two_copies(j):
                copy.wait()
            for w in range(4):
                part[w, y, x, c, :, half_a(j)] += in_two_a[w, :, packed(j)]
                part[w, y, x, c, :, half_b(j)] += in_two_b[w, :, packed(j)]
            for copy in line_copies(j):
                copy.start()

        @pl.when(jnp.logical_and(t >= 2, t < chunks + 2))
        def _():
            j = t - 2
            for copy in one_copies(j):
                copy.wait()
            for w in range(4):
                for v in range(2):
                    part[w, v, x, c, :, half_a(j)] += in_one_a[w, v, :, packed(j)]
                    part[w, y, v, c, :, half_b(j)] += in_one_b[w, v, :, packed(j)]
            for copy in two_copies(j):
                copy.start()

        @pl.when(jnp.logical_and(t >= 1, t < chunks + 1))
        def _():
            j = t - 1
            core_copy(j).wait()
            for w in range(4):
                for v in range(2):
                    for u in range(2):
                        part[w, v, u, c, :, both(j)] += in_core[w, v, u, :, both(j)]
            for copy in one_copies(j):
                copy.start()

        @pl.when(t < chunks)
        def _():
            rhs = rhs_ref[:, both(t)]

            def tile(w, carry):
                span = pl.ds(pl.multiple_of(w * quarter, quarter), quarter)
                if turned:
                    product = jnp.dot(lhs_ref[span, :], rhs, preferred_element_type=jnp.float32)
                else:
                    product = lax.dot_general(lhs_ref[:, span], rhs, FIRST_DIMS, preferred_element_type=jnp.float32)
                part[w, :, :, :, :, both(t)] = product.reshape(2, 2, 2, rows, CHUNK)
                return carry

            lax.fori_loop(0, 4, tile, 0)
            core_copy(t).start()

        return carry

    lax.fori_loop(0, chunks + 4, step, 0)


def product_scatter(lhs, rhs, collective_id, chunk=CHUNK, turned=False):
    total, depth = lhs.shape if turned else lhs.shape[::-1]
    features = rhs.shape[1]
    rows = total // 32
    chunks = features // chunk
    dma = pltpu.SemaphoreType.DMA
    f32 = jnp.float32
    return pl.pallas_call(
        functools.partial(scatter_kernel, chunk, turned),
        out_shape=jax.ShapeDtypeStruct((rows, features), f32),
        in_specs=[VMEM, VMEM], out_specs=VMEM,
        scratch_shapes=[pltpu.VMEM((4, 2, 2, 2, rows, features), f32), pltpu.VMEM((4, 2, 2, rows, features), f32),
                        pltpu.VMEM((4, 2, rows, features // 2), f32), pltpu.VMEM((4, 2, rows, features // 2), f32),
                        pltpu.VMEM((4, rows, features // 2), f32), pltpu.VMEM((4, rows, features // 2), f32),
                        pltpu.VMEM((3, rows, features), f32)]
                       + [dma((chunks,))] * 10 + [dma((3, chunks))] * 2,
        compiler_params=params(collective_id),
        cost_estimate=pl.CostEstimate(flops=2 * total * depth * features, bytes_accessed=4 * total * features,
                                      transcendentals=0),
        name="product_scatter",
    )(lhs, rhs)


def gather_kernel(block_ref, a_ref, b_ref, grad_a_ref, grad_b_ref, whole,
                  s3, r3, s2a, r2a, s2b, r2b, s1a, r1a, s1b, r1b, sc, rc):
    me, z, y, x, c = coords()
    core_peer = device_of(z, y, x, 1 - c)
    x_peer = device_of(z, y, 1 - x, c)
    y_peer = device_of(z, 1 - y, x, c)
    line = [(z + d) % 4 for d in range(1, 4)]
    line_peers = [device_of(p, y, x, c) for p in line]
    rows, features = block_ref.shape
    chunks = features // CHUNK
    greet([core_peer, x_peer, y_peer] + line_peers)

    def both(j):
        return pl.ds(pl.multiple_of(j * CHUNK, CHUNK), CHUNK)

    def half_a(j):
        return pl.ds(pl.multiple_of(j * CHUNK, HALF), HALF)

    def half_b(j):
        return pl.ds(pl.multiple_of(j * CHUNK + HALF, HALF), HALF)

    def line_copies(j):
        return [remote(block_ref.at[:, both(j)], whole.at[z, y, x, c, :, both(j)],
                       s3.at[d, j], r3.at[d, j], line_peers[d]) for d in range(3)]

    def two_copies(j):
        a, b = whole.at[:, y, x, c, :, half_a(j)], whole.at[:, y, x, c, :, half_b(j)]
        return (remote(a, a, s2a.at[j], r2a.at[j], y_peer), remote(b, b, s2b.at[j], r2b.at[j], x_peer))

    def one_copies(j):
        a, b = whole.at[:, :, x, c, :, half_a(j)], whole.at[:, y, :, c, :, half_b(j)]
        return (remote(a, a, s1a.at[j], r1a.at[j], x_peer), remote(b, b, s1b.at[j], r1b.at[j], y_peer))

    def core_copy(j):
        a = whole.at[:, :, :, c, :, both(j)]
        return remote(a, a, sc.at[j], rc.at[j], core_peer)

    whole[z, y, x, c] = block_ref[...]
    grad_a_ref[...] = jnp.zeros_like(grad_a_ref)

    def step(t, carry):
        @pl.when(t < chunks)
        def _():
            for copy in line_copies(t):
                copy.start()

        @pl.when(jnp.logical_and(t >= 1, t < chunks + 1))
        def _():
            for copy in line_copies(t - 1):
                copy.wait()
            for copy in two_copies(t - 1):
                copy.start()

        @pl.when(jnp.logical_and(t >= 2, t < chunks + 2))
        def _():
            for copy in two_copies(t - 2):
                copy.wait()
            for copy in one_copies(t - 2):
                copy.start()

        @pl.when(jnp.logical_and(t >= 3, t < chunks + 3))
        def _():
            for copy in one_copies(t - 3):
                copy.wait()
            core_copy(t - 3).start()

        @pl.when(t >= 4)
        def _():
            j = t - 4
            core_copy(j).wait()
            slab = whole[:, :, :, :, :, both(j)].reshape(32 * rows, CHUNK)
            grad_b_ref[:, both(j)] = jnp.dot(a_ref[...], slab, preferred_element_type=jnp.float32)
            grad_a_ref[...] += lax.dot_general(b_ref[:, both(j)], slab, (((1,), (1,)), ((), ())),
                                               preferred_element_type=jnp.float32)

        return carry

    lax.fori_loop(0, chunks + 4, step, 0)


def gather_products(block, embed_a, embed_b, collective_id):
    rows, features = block.shape
    chunks = features // CHUNK
    dma = pltpu.SemaphoreType.DMA
    shape = jax.ShapeDtypeStruct(embed_a.shape, jnp.float32)
    return pl.pallas_call(
        gather_kernel,
        out_shape=(shape, shape),
        in_specs=[VMEM] * 3, out_specs=(VMEM, VMEM),
        scratch_shapes=[pltpu.VMEM((4, 2, 2, 2, rows, features), jnp.bfloat16)]
                       + [dma((3, chunks))] * 2 + [dma((chunks,))] * 10,
        compiler_params=params(collective_id),
        cost_estimate=pl.CostEstimate(flops=4 * embed_a.size * features, bytes_accessed=4 * features * features,
                                      transcendentals=0),
        name="gather_products",
    )(block, embed_a, embed_b)


DEEP = 4
SLOTS = 3
STREAM = 18
BLOCK = 64


def descent_kernel(top_ref, act_two_ref, act_one_ref, feat_ref, w_three_ref, w_two_ref, normed_two_ref, normed_one_ref, aux_ref,
                   outs_ref, sums_ref,
                   rows, acts, weights, normed, masked, part, in_core, in_one_a, in_one_b, in_two_a, in_two_b, in_line,
                   part_sums, in_plane, own, in_rank, total,
                   load_rows, load_acts, load_weights, load_normed,
                   sc, rc, s1a, r1a, s1b, r1b, s2a, r2a, s2b, r2b, s3, r3,
                   free_core, free_1a, free_1b, free_2a, free_2b, free_line,
                   send_a, recv_a, send_b, recv_b, send_c, recv_c):
    me, z, y, x, c = coords()
    q = me % 8
    core_peer = device_of(z, y, x, 1 - c)
    x_peer = device_of(z, y, 1 - x, c)
    y_peer = device_of(z, 1 - y, x, c)
    line = [(z + d) % 4 for d in range(1, 4)]
    line_peers = [device_of(p, y, x, c) for p in line]
    line_sources = [device_of((z + 4 - d) % 4, y, x, c) for d in range(1, 4)]
    plane = [(q + d) % 8 for d in range(1, 8)]
    side = rows.shape[1] // 2
    count = side * 32

    copy_rows = pltpu.make_async_copy(top_ref, rows.at[0], load_rows)
    copy_act_two = pltpu.make_async_copy(act_two_ref, acts, load_acts)
    copy_act_one = pltpu.make_async_copy(act_one_ref, acts, load_acts)
    copy_w_three = pltpu.make_async_copy(w_three_ref, weights, load_weights)
    copy_w_two = pltpu.make_async_copy(w_two_ref, weights, load_weights)
    copy_normed_two = pltpu.make_async_copy(normed_two_ref, normed, load_normed)
    copy_normed_one = pltpu.make_async_copy(normed_one_ref, normed, load_normed)
    for copy in (copy_rows, copy_act_two, copy_w_three, copy_normed_two):
        copy.start()
    greet([z * 8 + p for p in plane] + line_peers)
    copy_rows.wait()

    def both(j):
        return pl.ds(pl.multiple_of(j * CHUNK, CHUNK), CHUNK)

    def signal(sem, peer):
        pl.semaphore_signal(sem, inc=1, device_id=(peer,), device_id_type=MESH)

    low, high = pl.ds(0, HALF), pl.ds(HALF, HALF)

    def core_copy(j):
        return remote(part.at[j % DEEP, :, :, :, 1 - c], in_core.at[j % SLOTS], sc.at[j % SLOTS], rc.at[j % SLOTS], core_peer)

    def one_copies(j):
        p, s = j % DEEP, j % SLOTS
        return (remote(part.at[p, :, :, 1 - x, c, :, low], in_one_a.at[s], s1a.at[s], r1a.at[s], x_peer),
                remote(part.at[p, :, 1 - y, :, c, :, high], in_one_b.at[s], s1b.at[s], r1b.at[s], y_peer))

    def two_copies(j):
        p, s = j % DEEP, j % SLOTS
        return (remote(part.at[p, :, 1 - y, x, c, :, low], in_two_a.at[s], s2a.at[s], r2a.at[s], y_peer),
                remote(part.at[p, :, y, 1 - x, c, :, high], in_two_b.at[s], s2b.at[s], r2b.at[s], x_peer))

    def line_copies(j):
        p, s = j % DEEP, j % SLOTS
        return [remote(part.at[p, w, y, x, c], in_line.at[s, d], s3.at[d, s], r3.at[d, s], line_peers[d])
                for d, w in enumerate(line)]

    def during(t, lag):
        return pl.when(jnp.logical_and(t >= lag, t < STREAM + lag))

    def stream_step(t):
        @during(t, 4)
        def _():
            j = t - 4
            p, s = j % DEEP, j % SLOTS
            for copy in line_copies(j):
                copy.wait()
            outs_ref[j] = (part[p, z, y, x, c] + in_line[s, 0]) + (in_line[s, 1] + in_line[s, 2])

            @pl.when(j < STREAM - SLOTS)
            def _():
                for d in range(3):
                    signal(free_line.at[d], line_sources[d])

        @during(t, 3)
        def _():
            j = t - 3
            p, s = j % DEEP, j % SLOTS
            for copy in two_copies(j):
                copy.wait()
            for w in range(4):
                part[p, w, y, x, c, :, low] += in_two_a[s, w]
                part[p, w, y, x, c, :, high] += in_two_b[s, w]

            @pl.when(j < STREAM - SLOTS)
            def _():
                signal(free_2a, y_peer)
                signal(free_2b, x_peer)

            @pl.when(j >= SLOTS)
            def _():
                for d in range(3):
                    pl.semaphore_wait(free_line.at[d], 1)

            for copy in line_copies(j):
                copy.start()

        @during(t, 2)
        def _():
            j = t - 2
            p, s = j % DEEP, j % SLOTS
            for copy in one_copies(j):
                copy.wait()
            for w in range(4):
                for v in range(2):
                    part[p, w, v, x, c, :, low] += in_one_a[s, w, v]
                    part[p, w, y, v, c, :, high] += in_one_b[s, w, v]

            @pl.when(j < STREAM - SLOTS)
            def _():
                signal(free_1a, x_peer)
                signal(free_1b, y_peer)

            @pl.when(j >= SLOTS)
            def _():
                pl.semaphore_wait(free_2a, 1)
                pl.semaphore_wait(free_2b, 1)

            for copy in two_copies(j):
                copy.start()

        @during(t, 1)
        def _():
            j = t - 1
            p, s = j % DEEP, j % SLOTS
            core_copy(j).wait()
            for w in range(4):
                for v in range(2):
                    for u in range(2):
                        part[p, w, v, u, c] += in_core[s, w, v, u]

            @pl.when(j < STREAM - SLOTS)
            def _():
                signal(free_core, core_peer)

            @pl.when(j >= SLOTS)
            def _():
                pl.semaphore_wait(free_1a, 1)
                pl.semaphore_wait(free_1b, 1)

            for copy in one_copies(j):
                copy.start()

        @pl.when(t < 16)
        def _():
            rhs = rows[t // 8, :, both(t % 8)]

            def tile(w, carry):
                product = lax.dot_general(acts[:, pl.ds(pl.multiple_of(w * 512, 512), 512)], rhs, FIRST_DIMS,
                                          preferred_element_type=jnp.float32)
                part[t % DEEP, w] = product.reshape(2, 2, 2, BLOCK, CHUNK)
                return carry

            lax.fori_loop(0, 4, tile, 0)

        @pl.when(jnp.logical_and(t >= 16, t < STREAM))
        def _():
            for k in range(4):
                product = jnp.dot(feat_ref[...], rows[2, :, both((t - 16) * 4 + k)], preferred_element_type=jnp.float32)
                part[t % DEEP, :, :, :, :, 16 * k:16 * k + 16, :] = product.reshape(4, 2, 2, 2, 16, CHUNK)

        @pl.when(t < STREAM)
        def _():
            @pl.when(t >= SLOTS)
            def _():
                pl.semaphore_wait(free_core, 1)

            core_copy(t).start()

    def pull(layer, j):
        cols = both(j)
        gain, shift = aux_ref[layer, 0:1, cols], aux_ref[layer, 1:2, cols]
        weight = weights[cols, :]
        for view in range(2):
            span = slice(view * side, (view + 1) * side)
            grad = lax.dot_general(rows[layer, span, :], weight, (((1,), (1,)), ((), ())),
                                   preferred_element_type=jnp.float32)
            hat = normed[span, cols]
            grad = jnp.where(gain * hat + shift > 0, grad, 0.0)
            masked[span, cols] = grad
            part_sums[view:view + 1, cols] = jnp.sum(grad, axis=0, keepdims=True)
            part_sums[2 + view:3 + view, cols] = jnp.sum(grad * hat, axis=0, keepdims=True)

    def push(layer, j):
        cols = both(j)
        gain = aux_ref[layer, 0:1, cols]
        for view in range(2):
            span = slice(view * side, (view + 1) * side)
            inv = aux_ref[layer, 2 + view:3 + view, cols]
            sum_one = sums_ref[layer, view:view + 1, cols] / count
            sum_two = sums_ref[layer, 2 + view:3 + view, cols] / count
            grad = inv * (masked[span, cols] - (sum_one + normed[span, cols] * sum_two))
            rows[layer + 1, span, cols] = (gain * grad).astype(jnp.bfloat16)

    def wide(k):
        return pl.ds(pl.multiple_of(k * CHUNK, CHUNK), CHUNK)

    def first_copies(layer):
        return [remote(part_sums.at[:, wide(p)], in_plane.at[layer, d], send_a.at[d], recv_a.at[layer, d], z * 8 + p)
                for d, p in enumerate(plane)]

    def second_copies(layer):
        return [remote(own, in_rank.at[layer, z], send_b.at[d], recv_b.at[layer, d], line_peers[d]) for d in range(3)]

    def third_copies(layer):
        return [remote(total, sums_ref.at[layer, :, wide(q)], send_c.at[d], recv_c.at[layer, d], z * 8 + p)
                for d, p in enumerate(plane)]

    def descend_step(t):
        layer, phase = t // 8, t % 8

        def at(k):
            return pl.when(jnp.logical_and(t < 16, phase == k))

        def pulls(lo, hi):
            def body(j, carry):
                pull(layer, j)
                return carry
            lax.fori_loop(lo, hi, body, 0)

        def pushes(lo, hi):
            def body(j, carry):
                push(layer, j)
                return carry
            lax.fori_loop(lo, hi, body, 0)

        @at(1)
        def _():
            copy_w_three.wait()
            copy_normed_two.wait()
            pulls(0, 2)

        @at(2)
        def _():
            pulls(2, 5)

        @at(3)
        def _():
            pulls(5, 8)
            for copy in first_copies(layer):
                copy.start()

        @pl.when(t == 3)
        def _():
            copy_w_two.start()

        @at(4)
        def _():
            acc = part_sums[:, wide(q)]
            for d, copy in enumerate(first_copies(layer)):
                copy.wait()
                acc = acc + in_plane[layer, d]
            own[...] = acc
            in_rank[layer, z] = acc
            for copy in second_copies(layer):
                copy.start()

        @at(5)
        def _():
            for copy in second_copies(layer):
                copy.wait()
            acc = (in_rank[layer, 0] + in_rank[layer, 1]) + (in_rank[layer, 2] + in_rank[layer, 3])
            total[...] = acc
            sums_ref[layer, :, wide(q)] = acc
            for copy in third_copies(layer):
                copy.start()

        @at(6)
        def _():
            for copy in third_copies(layer):
                copy.wait()
            pushes(0, 4)

        @at(7)
        def _():
            pushes(4, 8)

        @pl.when(t == 7)
        def _():
            copy_act_one.start()
            copy_normed_one.start()

    def step(t, carry):
        @pl.when(t == 0)
        def _():
            copy_act_two.wait()

        @pl.when(t == 8)
        def _():
            copy_act_one.wait()

        stream_step(t)
        descend_step(t)
        return carry

    lax.fori_loop(0, STREAM + 4, step, 0)


def descend(top, act_two, act_one, feat_t, w_three, w_two, normed_two, normed_one, aux, collective_id):
    depth, features = top.shape
    dma, regular = pltpu.SemaphoreType.DMA, pltpu.SemaphoreType.REGULAR
    f32, bf16 = jnp.float32, jnp.bfloat16
    away = pl.BlockSpec(memory_space=pltpu.HBM)
    return pl.pallas_call(
        descent_kernel,
        out_shape=(jax.ShapeDtypeStruct((STREAM, BLOCK, CHUNK), f32), jax.ShapeDtypeStruct((2, 4, features), f32)),
        in_specs=[away, away, away, VMEM, away, away, away, away, VMEM], out_specs=(VMEM, VMEM),
        scratch_shapes=[pltpu.VMEM((3, depth, features), bf16), pltpu.VMEM((depth, features), bf16),
                        pltpu.VMEM((features, features), bf16), pltpu.VMEM((depth, features), f32),
                        pltpu.VMEM((depth, features), f32),
                        pltpu.VMEM((DEEP, 4, 2, 2, 2, BLOCK, CHUNK), f32), pltpu.VMEM((SLOTS, 4, 2, 2, BLOCK, CHUNK), f32),
                        pltpu.VMEM((SLOTS, 4, 2, BLOCK, HALF), f32), pltpu.VMEM((SLOTS, 4, 2, BLOCK, HALF), f32),
                        pltpu.VMEM((SLOTS, 4, BLOCK, HALF), f32), pltpu.VMEM((SLOTS, 4, BLOCK, HALF), f32),
                        pltpu.VMEM((SLOTS, 3, BLOCK, CHUNK), f32),
                        pltpu.VMEM((4, features), f32), pltpu.VMEM((2, 7, 4, CHUNK), f32), pltpu.VMEM((4, CHUNK), f32),
                        pltpu.VMEM((2, 4, 4, CHUNK), f32), pltpu.VMEM((4, CHUNK), f32)]
                       + [dma] * 4 + [dma((SLOTS,))] * 10 + [dma((3, SLOTS))] * 2
                       + [regular] * 5 + [regular((3,))]
                       + [dma((7,)), dma((2, 7)), dma((3,)), dma((2, 3)), dma((7,)), dma((2, 7))],
        compiler_params=pltpu.CompilerParams(collective_id=collective_id, has_side_effects=True,
                                             vmem_limit_bytes=67043328),
        name="descend",
    )(top, act_two, act_one, feat_t, w_three, w_two, normed_two, normed_one, aux)


def norm_forward(values, total_rows, collective_id):
    part = jnp.concatenate([jnp.sum(values, axis=1), jnp.sum(values * values, axis=1)])
    col_sums = all_sums(part, collective_id).reshape(2, 2, -1)
    col_mean = col_sums[0] / total_rows
    inv_std = lax.rsqrt(col_sums[1] / total_rows - col_mean * col_mean + NORM_EPS)
    return (values - col_mean[:, None, :]) * inv_std[:, None, :], inv_std


def norm_backward(grad_out, normed, inv_std, total_rows, collective_id, extra=None):
    rows = [jnp.sum(grad_out, axis=1), jnp.sum(grad_out * normed, axis=1)]
    sums = all_sums(jnp.concatenate(rows if extra is None else rows + [extra]), collective_id)
    col_sums = sums[:4].reshape(2, 2, -1)
    grad_in = inv_std[:, None, :] * (grad_out - (col_sums[0][:, None, :] + normed * col_sums[1][:, None, :]) / total_rows)
    return grad_in, col_sums, sums[4:]


def solution(mesh):
    shards = mesh.shape[AXIS]

    def local_step(h_a, h_b, w_one, w_two, w_three, gain_one, shift_one, gain_two, shift_two, lam_off):
        me = lax.axis_index(AXIS)
        rows_dev = h_a.shape[0]
        total_rows = rows_dev * shards
        features = w_two.shape[0]
        feat_rows = jnp.concatenate([h_a, h_b], axis=0)
        in_rows = feat_rows.shape[1] // shards
        feat_t = jnp.pad(feat_rows.T.reshape(shards, in_rows, 2 * rows_dev), ((0, 0), (0, 16 - in_rows), (0, 0)))
        feat_t = feat_t.reshape(shards * 16, 2 * rows_dev)
        hidden_one = jnp.dot(feat_rows, w_one, preferred_element_type=jnp.float32).reshape(2, rows_dev, -1)
        normed_one, inv_one = norm_forward(hidden_one, total_rows, 0)
        pre_one = gain_one * normed_one + shift_one
        act_one = jax.nn.relu(pre_one).astype(jnp.bfloat16)
        hidden_two = jnp.dot(act_one, w_two, preferred_element_type=jnp.float32)
        normed_two, inv_two = norm_forward(hidden_two, total_rows, 1)
        pre_two = gain_two * normed_two + shift_two
        act_two = jax.nn.relu(pre_two).astype(jnp.bfloat16)
        proj_out = jnp.dot(act_two, w_three, preferred_element_type=jnp.float32)
        normed_out, inv_out = norm_forward(proj_out, total_rows, 2)
        embed_pair = normed_out.astype(jnp.bfloat16)
        corr_rows = product_scatter(embed_pair[0], embed_pair[1], 3) / total_rows
        block_rows = features // shards
        row_index = me * block_rows + jnp.arange(block_rows)
        diag_mask = row_index[:, None] == jnp.arange(features)[None, :]
        diag_gap = 1.0 - corr_rows
        loss_part = jnp.sum(jnp.where(diag_mask, diag_gap * diag_gap, lam_off * corr_rows * corr_rows),
                            axis=0, keepdims=True)
        grad_corr = jnp.where(diag_mask, -2.0 * diag_gap, 2.0 * lam_off * corr_rows)
        grad_scaled = (grad_corr / total_rows).astype(jnp.bfloat16)
        grad_embed = jnp.stack(gather_products(grad_scaled, embed_pair[0], embed_pair[1], 4))
        grad_proj, _, loss_row = norm_backward(grad_embed, normed_out, inv_out, total_rows, 5, loss_part)
        grad_proj = grad_proj.astype(jnp.bfloat16)
        loss_total = jnp.sum(loss_row)

        def flat(value):
            return value.reshape(2 * rows_dev, -1)

        aux = jnp.stack([jnp.stack([gain_two, shift_two, inv_two[0], inv_two[1]]),
                         jnp.stack([gain_one, shift_one, inv_one[0], inv_one[1]])])
        outs, sums = descend(flat(grad_proj), flat(act_two), flat(act_one), feat_t, w_three, w_two,
                             flat(normed_two), flat(normed_one), aux, 6)

        def block_of(chunk):
            return chunk.transpose(1, 0, 2).reshape(block_rows, features)

        grad_w_one = outs[16:].reshape(2, 4, 16, CHUNK).transpose(2, 0, 1, 3).reshape(16, features)[:in_rows]
        return (loss_total, grad_w_one, block_of(outs[8:16]), block_of(outs[:8]),
                sums[1, 2] + sums[1, 3], sums[1, 0] + sums[1, 1], sums[0, 2] + sums[0, 3], sums[0, 0] + sums[0, 1])

    row_spec = P(AXIS, None)
    whole_mat = P(None, None)
    whole_vec = P(None)
    return jax.shard_map(
        local_step, mesh=mesh,
        in_specs=(row_spec, row_spec, whole_mat, whole_mat, whole_mat,
                  whole_vec, whole_vec, whole_vec, whole_vec, P()),
        out_specs=(P(), row_spec, row_spec, row_spec, whole_vec, whole_vec, whole_vec, whole_vec),
        check_vma=False)
```

```python
import jax
import jax.numpy as jnp
from jax import lax
from jax.experimental import pallas as pl
from jax.experimental.pallas import tpu as pltpu
from jax.sharding import PartitionSpec as P

NORM_EPS = 1e-5
FIRST_DIMS = (((0,), (0,)), ((), ()))
MESH = pl.DeviceIdType.MESH
VMEM = pl.BlockSpec(memory_space=pltpu.VMEM)
AXIS = "data"
CHUNK = 256
HALF = 128
LIMIT = 67043328
DEEP = 4
SLOTS = 3
STREAM = 18
BLOCK = 64


def coords():
    me = lax.axis_index(AXIS)
    return me, me // 8, (me // 4) % 2, (me // 2) % 2, me % 2


def device_of(z, y, x, c):
    return ((z * 2 + y) * 2 + x) * 2 + c


def greet(peers):
    barrier = pltpu.get_barrier_semaphore()
    for peer in peers:
        pl.semaphore_signal(barrier, inc=1, device_id=(peer,), device_id_type=MESH)
    pl.semaphore_wait(barrier, len(peers))


def remote(src, dst, send_sem, recv_sem, peer):
    return pltpu.make_async_remote_copy(src_ref=src, dst_ref=dst, send_sem=send_sem, recv_sem=recv_sem,
                                        device_id=(peer,), device_id_type=MESH)


def params(collective_id):
    return pltpu.CompilerParams(collective_id=collective_id, has_side_effects=True, vmem_limit_bytes=LIMIT)


def both(j):
    return pl.ds(pl.multiple_of(j * CHUNK, CHUNK), CHUNK)


def stream_scratch():
    dma, regular, f32 = pltpu.SemaphoreType.DMA, pltpu.SemaphoreType.REGULAR, jnp.float32
    return [pltpu.VMEM((DEEP, 4, 2, 2, 2, BLOCK, CHUNK), f32), pltpu.VMEM((SLOTS, 4, 2, 2, BLOCK, CHUNK), f32),
            pltpu.VMEM((SLOTS, 4, 2, BLOCK, HALF), f32), pltpu.VMEM((SLOTS, 4, 2, BLOCK, HALF), f32),
            pltpu.VMEM((SLOTS, 4, BLOCK, HALF), f32), pltpu.VMEM((SLOTS, 4, BLOCK, HALF), f32),
            pltpu.VMEM((SLOTS, 3, BLOCK, CHUNK), f32)] + [dma((SLOTS,))] * 10 + [dma((3, SLOTS))] * 2 \
        + [regular] * 5 + [regular((3,))]


STREAM_REFS = 25


def peers_of(spot):
    z, y, x, c = spot
    line = [(z + d) % 4 for d in range(1, 4)]
    return (device_of(z, y, x, 1 - c), device_of(z, y, 1 - x, c), device_of(z, 1 - y, x, c),
            line, [device_of(p, y, x, c) for p in line])


def stream_of(length, spot, refs, produce, consume):
    (part, in_core, in_one_a, in_one_b, in_two_a, in_two_b, in_line,
     sc, rc, s1a, r1a, s1b, r1b, s2a, r2a, s2b, r2b, s3, r3,
     free_core, free_1a, free_1b, free_2a, free_2b, free_line) = refs
    z, y, x, c = spot
    core_peer, x_peer, y_peer, line, line_peers = peers_of(spot)
    line_sources = [device_of((z + 4 - d) % 4, y, x, c) for d in range(1, 4)]
    low, high = pl.ds(0, HALF), pl.ds(HALF, HALF)

    def signal(sem, peer):
        pl.semaphore_signal(sem, inc=1, device_id=(peer,), device_id_type=MESH)

    def core_copy(j):
        return remote(part.at[j % DEEP, :, :, :, 1 - c], in_core.at[j % SLOTS], sc.at[j % SLOTS], rc.at[j % SLOTS], core_peer)

    def one_copies(j):
        p, s = j % DEEP, j % SLOTS
        return (remote(part.at[p, :, :, 1 - x, c, :, low], in_one_a.at[s], s1a.at[s], r1a.at[s], x_peer),
                remote(part.at[p, :, 1 - y, :, c, :, high], in_one_b.at[s], s1b.at[s], r1b.at[s], y_peer))

    def two_copies(j):
        p, s = j % DEEP, j % SLOTS
        return (remote(part.at[p, :, 1 - y, x, c, :, low], in_two_a.at[s], s2a.at[s], r2a.at[s], y_peer),
                remote(part.at[p, :, y, 1 - x, c, :, high], in_two_b.at[s], s2b.at[s], r2b.at[s], x_peer))

    def line_copies(j):
        p, s = j % DEEP, j % SLOTS
        return [remote(part.at[p, w, y, x, c], in_line.at[s, d], s3.at[d, s], r3.at[d, s], line_peers[d])
                for d, w in enumerate(line)]

    def during(t, lag):
        return pl.when(jnp.logical_and(t >= lag, t < length + lag))

    def stream_step(t):
        @during(t, 4)
        def _():
            j = t - 4
            p, s = j % DEEP, j % SLOTS
            for copy in line_copies(j):
                copy.wait()
            consume(j, (part[p, z, y, x, c] + in_line[s, 0]) + (in_line[s, 1] + in_line[s, 2]))

            @pl.when(j < length - SLOTS)
            def _():
                for d in range(3):
                    signal(free_line.at[d], line_sources[d])

        @during(t, 3)
        def _():
            j = t - 3
            p, s = j % DEEP, j % SLOTS
            for copy in two_copies(j):
                copy.wait()
            for w in range(4):
                part[p, w, y, x, c, :, low] += in_two_a[s, w]
                part[p, w, y, x, c, :, high] += in_two_b[s, w]

            @pl.when(j < length - SLOTS)
            def _():
                signal(free_2a, y_peer)
                signal(free_2b, x_peer)

            @pl.when(j >= SLOTS)
            def _():
                for d in range(3):
                    pl.semaphore_wait(free_line.at[d], 1)

            for copy in line_copies(j):
                copy.start()

        @during(t, 2)
        def _():
            j = t - 2
            p, s = j % DEEP, j % SLOTS
            for copy in one_copies(j):
                copy.wait()
            for w in range(4):
                for v in range(2):
                    part[p, w, v, x, c, :, low] += in_one_a[s, w, v]
                    part[p, w, y, v, c, :, high] += in_one_b[s, w, v]

            @pl.when(j < length - SLOTS)
            def _():
                signal(free_1a, x_peer)
                signal(free_1b, y_peer)

            @pl.when(j >= SLOTS)
            def _():
                pl.semaphore_wait(free_2a, 1)
                pl.semaphore_wait(free_2b, 1)

            for copy in two_copies(j):
                copy.start()

        @during(t, 1)
        def _():
            j = t - 1
            p, s = j % DEEP, j % SLOTS
            core_copy(j).wait()
            for w in range(4):
                for v in range(2):
                    for u in range(2):
                        part[p, w, v, u, c] += in_core[s, w, v, u]

            @pl.when(j < length - SLOTS)
            def _():
                signal(free_core, core_peer)

            @pl.when(j >= SLOTS)
            def _():
                pl.semaphore_wait(free_1a, 1)
                pl.semaphore_wait(free_1b, 1)

            for copy in one_copies(j):
                copy.start()

        @pl.when(t < length)
        def _():
            produce(t, part.at[t % DEEP])

            @pl.when(t >= SLOTS)
            def _():
                pl.semaphore_wait(free_core, 1)

            core_copy(t).start()

    return stream_step


def exchange_scratch(count, rows, features):
    dma, f32 = pltpu.SemaphoreType.DMA, jnp.float32
    return [pltpu.VMEM((rows, features), f32), pltpu.VMEM((count, 7, rows, CHUNK), f32), pltpu.VMEM((rows, CHUNK), f32),
            pltpu.VMEM((count, 4, rows, CHUNK), f32), pltpu.VMEM((rows, CHUNK), f32), pltpu.VMEM((count, rows, features), f32),
            dma((7,)), dma((count, 7)), dma((3,)), dma((count, 3)), dma((7,)), dma((count, 7))]


EXCHANGE_REFS = 12


def exchange_of(spot, refs):
    part_sums, in_plane, own, in_rank, total, sums, send_a, recv_a, send_b, recv_b, send_c, recv_c = refs
    z, y, x, c = spot
    q = (y * 2 + x) * 2 + c
    plane = [(q + d) % 8 for d in range(1, 8)]
    line_peers = peers_of(spot)[4]

    def first_copies(k):
        return [remote(part_sums.at[:, both(p)], in_plane.at[k, d], send_a.at[d], recv_a.at[k, d], z * 8 + p)
                for d, p in enumerate(plane)]

    def second_copies(k):
        return [remote(own, in_rank.at[k, z], send_b.at[d], recv_b.at[k, d], line_peers[d]) for d in range(3)]

    def third_copies(k):
        return [remote(total, sums.at[k, :, both(q)], send_c.at[d], recv_c.at[k, d], z * 8 + p)
                for d, p in enumerate(plane)]

    def begin(k):
        for copy in first_copies(k):
            copy.start()

    def cross(k):
        acc = part_sums[:, both(q)]
        for d, copy in enumerate(first_copies(k)):
            copy.wait()
            acc = acc + in_plane[k, d]
        own[...] = acc
        in_rank[k, z] = acc
        for copy in second_copies(k):
            copy.start()

    def spread(k):
        for copy in second_copies(k):
            copy.wait()
        acc = (in_rank[k, 0] + in_rank[k, 1]) + (in_rank[k, 2] + in_rank[k, 3])
        total[...] = acc
        sums[k, :, both(q)] = acc
        for copy in third_copies(k):
            copy.start()

    def finish(k):
        for copy in third_copies(k):
            copy.wait()

    return begin, cross, spread, finish


def everyone(spot):
    z, y, x, c = spot
    q = (y * 2 + x) * 2 + c
    return [z * 8 + (q + d) % 8 for d in range(1, 8)] + peers_of(spot)[4]


def looped(count, body):
    def run(j, carry):
        body(j)
        return carry
    lax.fori_loop(0, count, run, 0)


def ascent_kernel(feat_ref, w_one_ref, w_two_ref, w_three_ref, aux_ref,
                  hat_one_ref, hat_two_ref, hat_three_ref, act_one_ref, act_two_ref, embed_ref, inv_ref,
                  weights, hats, acts, load_two, load_three, save_hat, save_act, *refs):
    me, *spot = coords()
    begin, cross, spread, finish = exchange_of(spot, refs)
    part_sums, sums = refs[0], refs[5]
    side = feat_ref.shape[0] // 2
    count = side * 32
    chunks = aux_ref.shape[1] // CHUNK
    load = [pltpu.make_async_copy(w_two_ref, weights.at[0], load_two),
            pltpu.make_async_copy(w_three_ref, weights.at[1], load_three)]
    for copy in load:
        copy.start()
    save_hats = [pltpu.make_async_copy(hats.at[k % 2], ref, save_hat.at[k])
                 for k, ref in enumerate((hat_one_ref, hat_two_ref, hat_three_ref))]
    save_acts = [pltpu.make_async_copy(acts.at[k % 2], ref, save_act.at[k])
                 for k, ref in enumerate((act_one_ref, act_two_ref, embed_ref))]
    for layer in range(3):
        if layer:
            load[layer - 1].wait()
        if layer == 2:
            save_hats[0].wait()
            save_acts[0].wait()
        source = feat_ref if layer == 0 else acts.at[layer - 1]
        weight = w_one_ref if layer == 0 else weights.at[layer - 1]
        hat_ref, act_ref = hats.at[layer % 2], acts.at[layer % 2]

        def product(j):
            cols = both(j)
            for view in range(2):
                span = slice(view * side, (view + 1) * side)
                value = jnp.dot(source[span, :], weight[:, cols], preferred_element_type=jnp.float32)
                hat_ref[span, cols] = value
                part_sums[view:view + 1, cols] = jnp.sum(value, axis=0, keepdims=True)
                part_sums[2 + view:3 + view, cols] = jnp.sum(value * value, axis=0, keepdims=True)

        def normalise(j):
            cols = both(j)
            for view in range(2):
                span = slice(view * side, (view + 1) * side)
                mean = sums[layer, view:view + 1, cols] / count
                inv = lax.rsqrt(sums[layer, 2 + view:3 + view, cols] / count - mean * mean + NORM_EPS)
                inv_ref[2 * layer + view:2 * layer + view + 1, cols] = inv
                hat = (hat_ref[span, cols] - mean) * inv
                hat_ref[span, cols] = hat
                if layer < 2:
                    gain, shift = aux_ref[2 * layer:2 * layer + 1, cols], aux_ref[2 * layer + 1:2 * layer + 2, cols]
                    hat = jnp.maximum(gain * hat + shift, 0.0)
                act_ref[span, cols] = hat.astype(jnp.bfloat16)

        looped(chunks, product)
        if layer == 0:
            greet(everyone(spot))
        begin(layer)
        cross(layer)
        spread(layer)
        finish(layer)
        looped(chunks, normalise)
        save_hats[layer].start()
        save_acts[layer].start()
    for k in (1, 2):
        save_hats[k].wait()
        save_acts[k].wait()


def ascend(feat, w_one, w_two, w_three, aux, collective_id):
    depth, features = feat.shape[0], w_two.shape[0]
    dma, f32, bf16 = pltpu.SemaphoreType.DMA, jnp.float32, jnp.bfloat16
    away = pl.BlockSpec(memory_space=pltpu.HBM)
    wide, narrow = jax.ShapeDtypeStruct((depth, features), f32), jax.ShapeDtypeStruct((depth, features), bf16)
    return pl.pallas_call(
        ascent_kernel,
        out_shape=(wide, wide, wide, narrow, narrow, narrow, jax.ShapeDtypeStruct((6, features), f32)),
        in_specs=[VMEM, VMEM, away, away, VMEM], out_specs=(away,) * 6 + (VMEM,),
        scratch_shapes=[pltpu.VMEM((2, features, features), bf16), pltpu.VMEM((2, depth, features), f32),
                        pltpu.VMEM((2, depth, features), bf16), dma, dma, dma((3,)), dma((3,))]
                       + exchange_scratch(3, 4, features),
        compiler_params=params(collective_id),
        name="ascend",
    )(feat, w_one, w_two, w_three, aux)


def corr_kernel(embed_ref, hat_ref, inv_ref, lam_ref, top_ref, loss_ref,
                grads, hats, mine, whole, load_hat, t3, u3, t2a, u2a, t2b, u2b, t1a, u1a, t1b, u1b, tc, uc, *refs):
    me, *spot = coords()
    z, y, x, c = spot
    core_peer, x_peer, y_peer, line, line_peers = peers_of(spot)
    stream_refs, exchange_refs = refs[:STREAM_REFS], refs[STREAM_REFS:]
    begin, cross, spread, finish = exchange_of(spot, exchange_refs)
    part_sums, sums = exchange_refs[0], exchange_refs[5]
    side, features = embed_ref.shape[0] // 2, embed_ref.shape[1]
    count = side * 32
    chunks = features // CHUNK
    first, second = slice(0, side), slice(side, 2 * side)
    load = pltpu.make_async_copy(hat_ref, hats, load_hat)
    load.start()
    grads[first, :] = jnp.zeros((side, features), jnp.float32)
    greet(everyone(spot))

    def half_a(j):
        return pl.ds(pl.multiple_of(j * CHUNK, HALF), HALF)

    def half_b(j):
        return pl.ds(pl.multiple_of(j * CHUNK + HALF, HALF), HALF)

    def line_copies(j):
        return [remote(mine.at[:, both(j)], whole.at[z, y, x, c, :, both(j)],
                       t3.at[d, j], u3.at[d, j], line_peers[d]) for d in range(3)]

    def two_copies(j):
        a, b = whole.at[:, y, x, c, :, half_a(j)], whole.at[:, y, x, c, :, half_b(j)]
        return (remote(a, a, t2a.at[j], u2a.at[j], y_peer), remote(b, b, t2b.at[j], u2b.at[j], x_peer))

    def one_copies(j):
        a, b = whole.at[:, :, x, c, :, half_a(j)], whole.at[:, y, :, c, :, half_b(j)]
        return (remote(a, a, t1a.at[j], u1a.at[j], x_peer), remote(b, b, t1b.at[j], u1b.at[j], y_peer))

    def core_copy(j):
        a = whole.at[:, :, :, c, :, both(j)]
        return remote(a, a, tc.at[j], uc.at[j], core_peer)

    def produce(j, slot):
        rhs = embed_ref[second, both(j)]

        def tile(w):
            product = lax.dot_general(embed_ref[first, pl.ds(pl.multiple_of(w * 512, 512), 512)], rhs, FIRST_DIMS,
                                      preferred_element_type=jnp.float32)
            slot[w] = product.reshape(2, 2, 2, BLOCK, CHUNK)

        looped(4, tile)

    def consume(j, block):
        corr = block / count
        lam = lam_ref[0:1, 0:1]
        row = me * BLOCK + lax.broadcasted_iota(jnp.int32, corr.shape, 0)
        col = j * CHUNK + lax.broadcasted_iota(jnp.int32, corr.shape, 1)
        gap = 1.0 - corr
        part_sums[4:5, both(j)] = jnp.sum(jnp.where(row == col, gap * gap, lam * corr * corr), axis=0, keepdims=True)
        grad = (jnp.where(row == col, -2.0 * gap, 2.0 * lam * corr) / count).astype(jnp.bfloat16)
        mine[:, both(j)] = grad
        whole[z, y, x, c, :, both(j)] = grad
        for copy in line_copies(j):
            copy.start()

    stream_step = stream_of(chunks, spot, stream_refs, produce, consume)

    def during(t, lag):
        return pl.when(jnp.logical_and(t >= lag, t < chunks + lag))

    def step(t):
        @during(t, 7)
        def _():
            for copy in one_copies(t - 7):
                copy.wait()
            core_copy(t - 7).start()

        @during(t, 6)
        def _():
            for copy in two_copies(t - 6):
                copy.wait()
            for copy in one_copies(t - 6):
                copy.start()

        @during(t, 5)
        def _():
            for copy in line_copies(t - 5):
                copy.wait()
            for copy in two_copies(t - 5):
                copy.start()

        stream_step(t)

        @during(t, 8)
        def _():
            j = t - 8
            core_copy(j).wait()
            slab = whole[:, :, :, :, :, both(j)].reshape(features, CHUNK)
            grads[second, both(j)] = jnp.dot(embed_ref[first, :], slab, preferred_element_type=jnp.float32)
            grads[first, :] += lax.dot_general(embed_ref[second, both(j)], slab, (((1,), (1,)), ((), ())),
                                               preferred_element_type=jnp.float32)

    looped(chunks + 8, step)
    load.wait()

    def add_up(j):
        cols = both(j)
        for view in range(2):
            span = slice(view * side, (view + 1) * side)
            grad = grads[span, cols]
            part_sums[view:view + 1, cols] = jnp.sum(grad, axis=0, keepdims=True)
            part_sums[2 + view:3 + view, cols] = jnp.sum(grad * hats[span, cols], axis=0, keepdims=True)

    looped(chunks, add_up)
    begin(0)
    cross(0)
    spread(0)
    finish(0)
    loss_ref[...] = sums[0, 4:5, :]

    def normalise(j):
        cols = both(j)
        for view in range(2):
            span = slice(view * side, (view + 1) * side)
            sum_one = sums[0, view:view + 1, cols] / count
            sum_two = sums[0, 2 + view:3 + view, cols] / count
            grad = inv_ref[view:view + 1, cols] * (grads[span, cols] - (sum_one + hats[span, cols] * sum_two))
            top_ref[span, cols] = grad.astype(jnp.bfloat16)

    looped(chunks, normalise)


def correlate(embed, hat, inv, lam, collective_id):
    depth, features = embed.shape
    chunks = features // CHUNK
    dma, f32, bf16 = pltpu.SemaphoreType.DMA, jnp.float32, jnp.bfloat16
    return pl.pallas_call(
        corr_kernel,
        out_shape=(jax.ShapeDtypeStruct((depth, features), bf16), jax.ShapeDtypeStruct((1, features), f32)),
        in_specs=[VMEM, pl.BlockSpec(memory_space=pltpu.HBM), VMEM, VMEM], out_specs=(VMEM, VMEM),
        scratch_shapes=[pltpu.VMEM((depth, features), f32), pltpu.VMEM((depth, features), f32),
                        pltpu.VMEM((BLOCK, features), bf16), pltpu.VMEM((4, 2, 2, 2, BLOCK, features), bf16), dma]
                       + [dma((3, chunks))] * 2 + [dma((chunks,))] * 10
                       + stream_scratch() + exchange_scratch(1, 5, features),
        compiler_params=params(collective_id),
        name="correlate",
    )(embed, hat, inv, lam)


def descent_kernel(top_ref, act_two_ref, act_one_ref, feat_ref, w_three_ref, w_two_ref, normed_two_ref, normed_one_ref, aux_ref,
                   outs_ref, sums_ref,
                   rows, acts, weights, normed, masked, load_rows, load_acts, load_weights, load_normed, *refs):
    me, *spot = coords()
    exchange_refs = refs[STREAM_REFS:]
    begin, cross, spread, finish = exchange_of(spot, exchange_refs)
    part_sums, sums = exchange_refs[0], exchange_refs[5]
    side = rows.shape[1] // 2
    count = side * 32

    copy_rows = pltpu.make_async_copy(top_ref, rows.at[0], load_rows)
    copy_act_two = pltpu.make_async_copy(act_two_ref, acts, load_acts)
    copy_act_one = pltpu.make_async_copy(act_one_ref, acts, load_acts)
    copy_w_three = pltpu.make_async_copy(w_three_ref, weights, load_weights)
    copy_w_two = pltpu.make_async_copy(w_two_ref, weights, load_weights)
    copy_normed_two = pltpu.make_async_copy(normed_two_ref, normed, load_normed)
    copy_normed_one = pltpu.make_async_copy(normed_one_ref, normed, load_normed)
    for copy in (copy_rows, copy_act_two, copy_w_three, copy_normed_two):
        copy.start()
    greet(everyone(spot))
    copy_rows.wait()

    def produce(t, slot):
        @pl.when(t < 16)
        def _():
            rhs = rows[t // 8, :, both(t % 8)]

            def tile(w):
                product = lax.dot_general(acts[:, pl.ds(pl.multiple_of(w * 512, 512), 512)], rhs, FIRST_DIMS,
                                          preferred_element_type=jnp.float32)
                slot[w] = product.reshape(2, 2, 2, BLOCK, CHUNK)

            looped(4, tile)

        @pl.when(t >= 16)
        def _():
            for k in range(4):
                product = jnp.dot(feat_ref[...], rows[2, :, both((t - 16) * 4 + k)], preferred_element_type=jnp.float32)
                slot[:, :, :, :, 16 * k:16 * k + 16, :] = product.reshape(4, 2, 2, 2, 16, CHUNK)

    def consume(j, block):
        outs_ref[j] = block

    stream_step = stream_of(STREAM, spot, refs[:STREAM_REFS], produce, consume)

    def pull(layer, j):
        cols = both(j)
        gain, shift = aux_ref[layer, 0:1, cols], aux_ref[layer, 1:2, cols]
        weight = weights[cols, :]
        for view in range(2):
            span = slice(view * side, (view + 1) * side)
            grad = lax.dot_general(rows[layer, span, :], weight, (((1,), (1,)), ((), ())),
                                   preferred_element_type=jnp.float32)
            hat = normed[span, cols]
            grad = jnp.where(gain * hat + shift > 0, grad, 0.0)
            masked[span, cols] = grad
            part_sums[view:view + 1, cols] = jnp.sum(grad, axis=0, keepdims=True)
            part_sums[2 + view:3 + view, cols] = jnp.sum(grad * hat, axis=0, keepdims=True)

    def push(layer, j):
        cols = both(j)
        gain = aux_ref[layer, 0:1, cols]
        for view in range(2):
            span = slice(view * side, (view + 1) * side)
            inv = aux_ref[layer, 2 + view:3 + view, cols]
            sum_one = sums[layer, view:view + 1, cols] / count
            sum_two = sums[layer, 2 + view:3 + view, cols] / count
            grad = inv * (masked[span, cols] - (sum_one + normed[span, cols] * sum_two))
            rows[layer + 1, span, cols] = (gain * grad).astype(jnp.bfloat16)

    def descend_step(t):
        layer, phase = t // 8, t % 8

        def at(k):
            return pl.when(jnp.logical_and(t < 16, phase == k))

        def pulls(lo, hi):
            def body(j, carry):
                pull(layer, j)
                return carry
            lax.fori_loop(lo, hi, body, 0)

        def pushes(lo, hi):
            def body(j, carry):
                push(layer, j)
                return carry
            lax.fori_loop(lo, hi, body, 0)

        @at(1)
        def _():
            copy_w_three.wait()
            copy_normed_two.wait()
            pulls(0, 2)

        @at(2)
        def _():
            pulls(2, 5)

        @at(3)
        def _():
            pulls(5, 8)
            begin(layer)

        @pl.when(t == 3)
        def _():
            copy_w_two.start()

        @at(4)
        def _():
            cross(layer)

        @at(5)
        def _():
            spread(layer)

        @at(6)
        def _():
            finish(layer)
            pushes(0, 4)

        @at(7)
        def _():
            pushes(4, 8)

        @pl.when(t == 7)
        def _():
            copy_act_one.start()
            copy_normed_one.start()

    def step(t, carry):
        @pl.when(t == 0)
        def _():
            copy_act_two.wait()

        @pl.when(t == 8)
        def _():
            copy_act_one.wait()

        stream_step(t)
        descend_step(t)
        return carry

    lax.fori_loop(0, STREAM + 4, step, 0)
    sums_ref[...] = sums[...]


def descend(top, act_two, act_one, feat_t, w_three, w_two, normed_two, normed_one, aux, collective_id):
    depth, features = top.shape
    dma, f32, bf16 = pltpu.SemaphoreType.DMA, jnp.float32, jnp.bfloat16
    away = pl.BlockSpec(memory_space=pltpu.HBM)
    return pl.pallas_call(
        descent_kernel,
        out_shape=(jax.ShapeDtypeStruct((STREAM, BLOCK, CHUNK), f32), jax.ShapeDtypeStruct((2, 4, features), f32)),
        in_specs=[away, away, away, VMEM, away, away, away, away, VMEM], out_specs=(VMEM, VMEM),
        scratch_shapes=[pltpu.VMEM((3, depth, features), bf16), pltpu.VMEM((depth, features), bf16),
                        pltpu.VMEM((features, features), bf16), pltpu.VMEM((depth, features), f32),
                        pltpu.VMEM((depth, features), f32),
                        ] + [dma] * 4 + stream_scratch() + exchange_scratch(2, 4, features),
        compiler_params=params(collective_id),
        name="descend",
    )(top, act_two, act_one, feat_t, w_three, w_two, normed_two, normed_one, aux)


def solution(mesh):
    shards = mesh.shape[AXIS]

    def local_step(h_a, h_b, w_one, w_two, w_three, gain_one, shift_one, gain_two, shift_two, lam_off):
        rows_dev = h_a.shape[0]
        features = w_two.shape[0]
        block_rows = features // shards
        feat_rows = jnp.concatenate([h_a, h_b], axis=0)
        in_rows = feat_rows.shape[1] // shards
        feat_t = jnp.pad(feat_rows.T.reshape(shards, in_rows, 2 * rows_dev), ((0, 0), (0, 16 - in_rows), (0, 0)))
        feat_t = feat_t.reshape(shards * 16, 2 * rows_dev)
        hat_one, hat_two, hat_out, act_one, act_two, embed, inv = ascend(
            feat_rows, w_one, w_two, w_three, jnp.stack([gain_one, shift_one, gain_two, shift_two]), 0)
        top, loss_row = correlate(embed, hat_out, inv[4:], jnp.full((1, 128), lam_off), 1)
        aux = jnp.stack([jnp.stack([gain_two, shift_two, inv[2], inv[3]]), jnp.stack([gain_one, shift_one, inv[0], inv[1]])])
        outs, sums = descend(top, act_two, act_one, feat_t, w_three, w_two, hat_two, hat_one, aux, 2)

        def block_of(chunk):
            return chunk.transpose(1, 0, 2).reshape(block_rows, features)

        grad_w_one = outs[16:].reshape(2, 4, 16, CHUNK).transpose(2, 0, 1, 3).reshape(16, features)[:in_rows]
        return (jnp.sum(loss_row), grad_w_one, block_of(outs[8:16]), block_of(outs[:8]),
                sums[1, 2] + sums[1, 3], sums[1, 0] + sums[1, 1], sums[0, 2] + sums[0, 3], sums[0, 0] + sums[0, 1])

    row_spec = P(AXIS, None)
    whole_mat = P(None, None)
    whole_vec = P(None)
    return jax.shard_map(
        local_step, mesh=mesh,
        in_specs=(row_spec, row_spec, whole_mat, whole_mat, whole_mat,
                  whole_vec, whole_vec, whole_vec, whole_vec, P()),
        out_specs=(P(), row_spec, row_spec, row_spec, whole_vec, whole_vec, whole_vec, whole_vec),
        check_vma=False)
```

```python
import jax
import jax.numpy as jnp
from jax import lax
from jax.experimental import pallas as pl
from jax.experimental.pallas import tpu as pltpu
from jax.sharding import PartitionSpec as P

NORM_EPS = 1e-5
FIRST_DIMS = (((0,), (0,)), ((), ()))
MESH = pl.DeviceIdType.MESH
VMEM = pl.BlockSpec(memory_space=pltpu.VMEM)
AXIS = "data"
CHUNK = 256
HALF = 128
LIMIT = 67043328
DEEP = 4
SLOTS = 3
STREAM = 18
BLOCK = 64


def coords():
    me = lax.axis_index(AXIS)
    return me, me // 8, (me // 4) % 2, (me // 2) % 2, me % 2


def device_of(z, y, x, c):
    return ((z * 2 + y) * 2 + x) * 2 + c


def greet(peers):
    barrier = pltpu.get_barrier_semaphore()
    for peer in peers:
        pl.semaphore_signal(barrier, inc=1, device_id=(peer,), device_id_type=MESH)
    pl.semaphore_wait(barrier, len(peers))


def remote(src, dst, send_sem, recv_sem, peer):
    return pltpu.make_async_remote_copy(src_ref=src, dst_ref=dst, send_sem=send_sem, recv_sem=recv_sem,
                                        device_id=(peer,), device_id_type=MESH)


def params(collective_id):
    return pltpu.CompilerParams(collective_id=collective_id, has_side_effects=True, vmem_limit_bytes=LIMIT)


def both(j):
    return pl.ds(pl.multiple_of(j * CHUNK, CHUNK), CHUNK)


def stream_scratch():
    dma, regular, f32 = pltpu.SemaphoreType.DMA, pltpu.SemaphoreType.REGULAR, jnp.float32
    return [pltpu.VMEM((DEEP, 4, 2, 2, 2, BLOCK, CHUNK), f32), pltpu.VMEM((SLOTS, 4, 2, 2, BLOCK, CHUNK), f32),
            pltpu.VMEM((SLOTS, 4, 2, BLOCK, HALF), f32), pltpu.VMEM((SLOTS, 4, 2, BLOCK, HALF), f32),
            pltpu.VMEM((SLOTS, 4, BLOCK, HALF), f32), pltpu.VMEM((SLOTS, 4, BLOCK, HALF), f32),
            pltpu.VMEM((SLOTS, 3, BLOCK, CHUNK), f32)] + [dma((SLOTS,))] * 10 + [dma((3, SLOTS))] * 2 \
        + [regular] * 5 + [regular((3,))]


STREAM_REFS = 25


def peers_of(spot):
    z, y, x, c = spot
    line = [(z + d) % 4 for d in range(1, 4)]
    return (device_of(z, y, x, 1 - c), device_of(z, y, 1 - x, c), device_of(z, 1 - y, x, c),
            line, [device_of(p, y, x, c) for p in line])


def stream_of(length, spot, refs, produce, consume):
    (part, in_core, in_one_a, in_one_b, in_two_a, in_two_b, in_line,
     sc, rc, s1a, r1a, s1b, r1b, s2a, r2a, s2b, r2b, s3, r3,
     free_core, free_1a, free_1b, free_2a, free_2b, free_line) = refs
    z, y, x, c = spot
    core_peer, x_peer, y_peer, line, line_peers = peers_of(spot)
    line_sources = [device_of((z + 4 - d) % 4, y, x, c) for d in range(1, 4)]
    low, high = pl.ds(0, HALF), pl.ds(HALF, HALF)

    def signal(sem, peer):
        pl.semaphore_signal(sem, inc=1, device_id=(peer,), device_id_type=MESH)

    def core_copy(j):
        return remote(part.at[j % DEEP, :, :, :, 1 - c], in_core.at[j % SLOTS], sc.at[j % SLOTS], rc.at[j % SLOTS], core_peer)

    def one_copies(j):
        p, s = j % DEEP, j % SLOTS
        return (remote(part.at[p, :, :, 1 - x, c, :, low], in_one_a.at[s], s1a.at[s], r1a.at[s], x_peer),
                remote(part.at[p, :, 1 - y, :, c, :, high], in_one_b.at[s], s1b.at[s], r1b.at[s], y_peer))

    def two_copies(j):
        p, s = j % DEEP, j % SLOTS
        return (remote(part.at[p, :, 1 - y, x, c, :, low], in_two_a.at[s], s2a.at[s], r2a.at[s], y_peer),
                remote(part.at[p, :, y, 1 - x, c, :, high], in_two_b.at[s], s2b.at[s], r2b.at[s], x_peer))

    def line_copies(j):
        p, s = j % DEEP, j % SLOTS
        return [remote(part.at[p, w, y, x, c], in_line.at[s, d], s3.at[d, s], r3.at[d, s], line_peers[d])
                for d, w in enumerate(line)]

    def during(t, lag):
        return pl.when(jnp.logical_and(t >= lag, t < length + lag))

    def stream_step(t):
        @during(t, 1)
        def _():
            j = t - 1
            p, s = j % DEEP, j % SLOTS
            core_copy(j).wait()
            for w in range(4):
                for v in range(2):
                    for u in range(2):
                        part[p, w, v, u, c] += in_core[s, w, v, u]

            @pl.when(j < length - SLOTS)
            def _():
                signal(free_core, core_peer)

            @pl.when(j >= SLOTS)
            def _():
                pl.semaphore_wait(free_1a, 1)
                pl.semaphore_wait(free_1b, 1)

            for copy in one_copies(j):
                copy.start()

        @during(t, 2)
        def _():
            j = t - 2
            p, s = j % DEEP, j % SLOTS
            for copy in one_copies(j):
                copy.wait()
            for w in range(4):
                for v in range(2):
                    part[p, w, v, x, c, :, low] += in_one_a[s, w, v]
                    part[p, w, y, v, c, :, high] += in_one_b[s, w, v]

            @pl.when(j < length - SLOTS)
            def _():
                signal(free_1a, x_peer)
                signal(free_1b, y_peer)

            @pl.when(j >= SLOTS)
            def _():
                pl.semaphore_wait(free_2a, 1)
                pl.semaphore_wait(free_2b, 1)

            for copy in two_copies(j):
                copy.start()

        @during(t, 3)
        def _():
            j = t - 3
            p, s = j % DEEP, j % SLOTS
            for copy in two_copies(j):
                copy.wait()
            for w in range(4):
                part[p, w, y, x, c, :, low] += in_two_a[s, w]
                part[p, w, y, x, c, :, high] += in_two_b[s, w]

            @pl.when(j < length - SLOTS)
            def _():
                signal(free_2a, y_peer)
                signal(free_2b, x_peer)

            @pl.when(j >= SLOTS)
            def _():
                for d in range(3):
                    pl.semaphore_wait(free_line.at[d], 1)

            for copy in line_copies(j):
                copy.start()

        @during(t, 4)
        def _():
            j = t - 4
            p, s = j % DEEP, j % SLOTS
            for copy in line_copies(j):
                copy.wait()
            consume(j, (part[p, z, y, x, c] + in_line[s, 0]) + (in_line[s, 1] + in_line[s, 2]))

            @pl.when(j < length - SLOTS)
            def _():
                for d in range(3):
                    signal(free_line.at[d], line_sources[d])

        @pl.when(t < length)
        def _():
            produce(t, part.at[t % DEEP])

            @pl.when(t >= SLOTS)
            def _():
                pl.semaphore_wait(free_core, 1)

            core_copy(t).start()

    return stream_step


def exchange_scratch(count, rows, features):
    dma, f32 = pltpu.SemaphoreType.DMA, jnp.float32
    return [pltpu.VMEM((rows, features), f32), pltpu.VMEM((count, 7, rows, CHUNK), f32), pltpu.VMEM((rows, CHUNK), f32),
            pltpu.VMEM((count, 4, rows, CHUNK), f32), pltpu.VMEM((rows, CHUNK), f32), pltpu.VMEM((count, rows, features), f32),
            dma((7,)), dma((count, 7)), dma((3,)), dma((count, 3)), dma((7,)), dma((count, 7))]


EXCHANGE_REFS = 12


def exchange_of(spot, refs):
    part_sums, in_plane, own, in_rank, total, sums, send_a, recv_a, send_b, recv_b, send_c, recv_c = refs
    z, y, x, c = spot
    q = (y * 2 + x) * 2 + c
    plane = [(q + d) % 8 for d in range(1, 8)]
    line_peers = peers_of(spot)[4]

    def first_copies(k):
        return [remote(part_sums.at[:, both(p)], in_plane.at[k, d], send_a.at[d], recv_a.at[k, d], z * 8 + p)
                for d, p in enumerate(plane)]

    def second_copies(k):
        return [remote(own, in_rank.at[k, z], send_b.at[d], recv_b.at[k, d], line_peers[d]) for d in range(3)]

    def third_copies(k):
        return [remote(total, sums.at[k, :, both(q)], send_c.at[d], recv_c.at[k, d], z * 8 + p)
                for d, p in enumerate(plane)]

    def begin(k):
        for copy in first_copies(k):
            copy.start()

    def cross(k):
        acc = part_sums[:, both(q)]
        for d, copy in enumerate(first_copies(k)):
            copy.wait()
            acc = acc + in_plane[k, d]
        own[...] = acc
        in_rank[k, z] = acc
        for copy in second_copies(k):
            copy.start()

    def spread(k):
        for copy in second_copies(k):
            copy.wait()
        acc = (in_rank[k, 0] + in_rank[k, 1]) + (in_rank[k, 2] + in_rank[k, 3])
        total[...] = acc
        sums[k, :, both(q)] = acc
        for copy in third_copies(k):
            copy.start()

    def finish(k):
        for copy in third_copies(k):
            copy.wait()

    return begin, cross, spread, finish


def everyone(spot):
    z, y, x, c = spot
    q = (y * 2 + x) * 2 + c
    return [z * 8 + (q + d) % 8 for d in range(1, 8)] + peers_of(spot)[4]


def looped(count, body):
    def run(j, carry):
        body(j)
        return carry
    lax.fori_loop(0, count, run, 0)


def ascent_kernel(view_a_ref, view_b_ref, w_one_ref, w_two_ref, w_three_ref, aux_ref,
                  hat_one_ref, hat_two_ref, hat_three_ref, act_one_ref, act_two_ref, embed_ref, inv_ref,
                  weights, hats, acts, load_two, load_three, save_hat, save_act, *refs):
    me, *spot = coords()
    begin, cross, spread, finish = exchange_of(spot, refs)
    part_sums, sums = refs[0], refs[5]
    side = view_a_ref.shape[0]
    count = side * 32
    chunks = aux_ref.shape[2] // CHUNK
    load = [pltpu.make_async_copy(w_two_ref, weights.at[0], load_two),
            pltpu.make_async_copy(w_three_ref, weights.at[1], load_three)]
    for copy in load:
        copy.start()
    save_hats = [pltpu.make_async_copy(hats.at[k % 2], ref, save_hat.at[k])
                 for k, ref in enumerate((hat_one_ref, hat_two_ref, hat_three_ref))]
    save_acts = [pltpu.make_async_copy(acts.at[k % 2], ref, save_act.at[k])
                 for k, ref in enumerate((act_one_ref, act_two_ref, embed_ref))]
    for layer in range(3):
        if layer:
            load[layer - 1].wait()
        if layer == 2:
            save_hats[0].wait()
            save_acts[0].wait()
        weight = w_one_ref if layer == 0 else weights.at[layer - 1]
        hat_ref, act_ref = hats.at[layer % 2], acts.at[layer % 2]

        def product(j):
            cols = both(j)
            for view in range(2):
                span = slice(view * side, (view + 1) * side)
                source = (view_a_ref, view_b_ref)[view][...] if layer == 0 else acts[layer - 1, span, :]
                value = jnp.dot(source, weight[:, cols], preferred_element_type=jnp.float32)
                hat_ref[span, cols] = value
                part_sums[view:view + 1, cols] = jnp.sum(value, axis=0, keepdims=True)
                part_sums[2 + view:3 + view, cols] = jnp.sum(value * value, axis=0, keepdims=True)

        def normalise(j):
            cols = both(j)
            for view in range(2):
                span = slice(view * side, (view + 1) * side)
                mean = sums[layer, view:view + 1, cols] / count
                inv = lax.rsqrt(sums[layer, 2 + view:3 + view, cols] / count - mean * mean + NORM_EPS)
                inv_ref[layer, view:view + 1, cols] = inv
                hat = (hat_ref[span, cols] - mean) * inv
                hat_ref[span, cols] = hat
                if layer < 2:
                    gain, shift = aux_ref[layer, 0:1, cols], aux_ref[layer, 1:2, cols]
                    hat = jnp.maximum(gain * hat + shift, 0.0)
                act_ref[span, cols] = hat.astype(jnp.bfloat16)

        looped(chunks, product)
        if layer == 0:
            greet(everyone(spot))
        begin(layer)
        cross(layer)
        spread(layer)
        finish(layer)
        looped(chunks, normalise)
        save_hats[layer].start()
        save_acts[layer].start()
    for k in (1, 2):
        save_hats[k].wait()
        save_acts[k].wait()


def ascend(view_a, view_b, w_one, w_two, w_three, aux, collective_id):
    depth, features = 2 * view_a.shape[0], w_two.shape[0]
    dma, f32, bf16 = pltpu.SemaphoreType.DMA, jnp.float32, jnp.bfloat16
    away = pl.BlockSpec(memory_space=pltpu.HBM)
    wide, narrow = jax.ShapeDtypeStruct((depth, features), f32), jax.ShapeDtypeStruct((depth, features), bf16)
    return pl.pallas_call(
        ascent_kernel,
        out_shape=(wide, wide, wide, narrow, narrow, narrow, jax.ShapeDtypeStruct((3, 2, features), f32)),
        in_specs=[VMEM, VMEM, VMEM, away, away, VMEM], out_specs=(away,) * 6 + (VMEM,),
        scratch_shapes=[pltpu.VMEM((2, features, features), bf16), pltpu.VMEM((2, depth, features), f32),
                        pltpu.VMEM((2, depth, features), bf16), dma, dma, dma((3,)), dma((3,))]
                       + exchange_scratch(3, 4, features),
        compiler_params=params(collective_id),
        name="ascend",
    )(view_a, view_b, w_one, w_two, w_three, aux)


def corr_kernel(embed_ref, hat_ref, inv_ref, lam_ref, top_ref, loss_ref,
                grads, hats, mine, whole, load_hat, t3, u3, t2a, u2a, t2b, u2b, t1a, u1a, t1b, u1b, tc, uc, *refs):
    me, *spot = coords()
    z, y, x, c = spot
    core_peer, x_peer, y_peer, line, line_peers = peers_of(spot)
    stream_refs, exchange_refs = refs[:STREAM_REFS], refs[STREAM_REFS:]
    begin, cross, spread, finish = exchange_of(spot, exchange_refs)
    part_sums, sums = exchange_refs[0], exchange_refs[5]
    side, features = embed_ref.shape[0] // 2, embed_ref.shape[1]
    count = side * 32
    chunks = features // CHUNK
    first, second = slice(0, side), slice(side, 2 * side)
    load = pltpu.make_async_copy(hat_ref, hats, load_hat)
    load.start()
    grads[first, :] = jnp.zeros((side, features), jnp.float32)
    greet(everyone(spot))

    def half_a(j):
        return pl.ds(pl.multiple_of(j * CHUNK, HALF), HALF)

    def half_b(j):
        return pl.ds(pl.multiple_of(j * CHUNK + HALF, HALF), HALF)

    def line_copies(j):
        return [remote(mine.at[:, both(j)], whole.at[z, y, x, c, :, both(j)],
                       t3.at[d, j], u3.at[d, j], line_peers[d]) for d in range(3)]

    def two_copies(j):
        a, b = whole.at[:, y, x, c, :, half_a(j)], whole.at[:, y, x, c, :, half_b(j)]
        return (remote(a, a, t2a.at[j], u2a.at[j], y_peer), remote(b, b, t2b.at[j], u2b.at[j], x_peer))

    def one_copies(j):
        a, b = whole.at[:, :, x, c, :, half_a(j)], whole.at[:, y, :, c, :, half_b(j)]
        return (remote(a, a, t1a.at[j], u1a.at[j], x_peer), remote(b, b, t1b.at[j], u1b.at[j], y_peer))

    def core_copy(j):
        a = whole.at[:, :, :, c, :, both(j)]
        return remote(a, a, tc.at[j], uc.at[j], core_peer)

    def produce(j, slot):
        rhs = embed_ref[second, both(j)]

        def tile(w):
            product = lax.dot_general(embed_ref[first, pl.ds(pl.multiple_of(w * 512, 512), 512)], rhs, FIRST_DIMS,
                                      preferred_element_type=jnp.float32)
            slot[w] = product.reshape(2, 2, 2, BLOCK, CHUNK)

        looped(4, tile)

    def consume(j, block):
        corr = block / count
        lam = lam_ref[0:1, 0:1]
        row = me * BLOCK + lax.broadcasted_iota(jnp.int32, corr.shape, 0)
        col = j * CHUNK + lax.broadcasted_iota(jnp.int32, corr.shape, 1)
        gap = 1.0 - corr
        part_sums[4:5, both(j)] = jnp.sum(jnp.where(row == col, gap * gap, lam * corr * corr), axis=0, keepdims=True)
        grad = (jnp.where(row == col, -2.0 * gap, 2.0 * lam * corr) / count).astype(jnp.bfloat16)
        mine[:, both(j)] = grad
        whole[z, y, x, c, :, both(j)] = grad
        for copy in line_copies(j):
            copy.start()

    stream_step = stream_of(chunks, spot, stream_refs, produce, consume)

    def during(t, lag):
        return pl.when(jnp.logical_and(t >= lag, t < chunks + lag))

    def step(t):
        stream_step(t)

        @during(t, 5)
        def _():
            for copy in line_copies(t - 5):
                copy.wait()
            for copy in two_copies(t - 5):
                copy.start()

        @during(t, 6)
        def _():
            for copy in two_copies(t - 6):
                copy.wait()
            for copy in one_copies(t - 6):
                copy.start()

        @during(t, 7)
        def _():
            for copy in one_copies(t - 7):
                copy.wait()
            core_copy(t - 7).start()

        @during(t, 8)
        def _():
            j = t - 8
            core_copy(j).wait()
            slab = whole[:, :, :, :, :, both(j)].reshape(features, CHUNK)
            grads[second, both(j)] = jnp.dot(embed_ref[first, :], slab, preferred_element_type=jnp.float32)
            grads[first, :] += lax.dot_general(embed_ref[second, both(j)], slab, (((1,), (1,)), ((), ())),
                                               preferred_element_type=jnp.float32)

    looped(chunks + 8, step)
    load.wait()

    def add_up(j):
        cols = both(j)
        for view in range(2):
            span = slice(view * side, (view + 1) * side)
            grad = grads[span, cols]
            part_sums[view:view + 1, cols] = jnp.sum(grad, axis=0, keepdims=True)
            part_sums[2 + view:3 + view, cols] = jnp.sum(grad * hats[span, cols], axis=0, keepdims=True)

    looped(chunks, add_up)
    begin(0)
    cross(0)
    spread(0)
    finish(0)
    loss_ref[...] = jnp.sum(sums[0, 4:5, :], axis=1, keepdims=True)

    def normalise(j):
        cols = both(j)
        for view in range(2):
            span = slice(view * side, (view + 1) * side)
            sum_one = sums[0, view:view + 1, cols] / count
            sum_two = sums[0, 2 + view:3 + view, cols] / count
            grad = inv_ref[2, view:view + 1, cols] * (grads[span, cols] - (sum_one + hats[span, cols] * sum_two))
            top_ref[span, cols] = grad.astype(jnp.bfloat16)

    looped(chunks, normalise)


def correlate(embed, hat, inv, lam, collective_id):
    depth, features = embed.shape
    chunks = features // CHUNK
    dma, f32, bf16 = pltpu.SemaphoreType.DMA, jnp.float32, jnp.bfloat16
    return pl.pallas_call(
        corr_kernel,
        out_shape=(jax.ShapeDtypeStruct((depth, features), bf16), jax.ShapeDtypeStruct((1, 1), f32)),
        in_specs=[VMEM, pl.BlockSpec(memory_space=pltpu.HBM), VMEM, VMEM], out_specs=(VMEM, VMEM),
        scratch_shapes=[pltpu.VMEM((depth, features), f32), pltpu.VMEM((depth, features), f32),
                        pltpu.VMEM((BLOCK, features), bf16), pltpu.VMEM((4, 2, 2, 2, BLOCK, features), bf16), dma]
                       + [dma((3, chunks))] * 2 + [dma((chunks,))] * 10
                       + stream_scratch() + exchange_scratch(1, 5, features),
        compiler_params=params(collective_id),
        name="correlate",
    )(embed, hat, inv, lam)


def descent_kernel(top_ref, act_two_ref, act_one_ref, feat_ref, w_three_ref, w_two_ref, normed_two_ref, normed_one_ref, aux_ref, inv_ref,
                   out_three_ref, out_two_ref, out_one_ref, sums_ref,
                   rows, acts, weights, normed, masked, load_rows, load_acts, load_weights, load_normed, *refs):
    me, *spot = coords()
    exchange_refs = refs[STREAM_REFS:]
    begin, cross, spread, finish = exchange_of(spot, exchange_refs)
    part_sums, sums = exchange_refs[0], exchange_refs[5]
    side = rows.shape[1] // 2
    count = side * 32

    copy_rows = pltpu.make_async_copy(top_ref, rows.at[0], load_rows)
    copy_act_two = pltpu.make_async_copy(act_two_ref, acts, load_acts)
    copy_act_one = pltpu.make_async_copy(act_one_ref, acts, load_acts)
    copy_w_three = pltpu.make_async_copy(w_three_ref, weights, load_weights)
    copy_w_two = pltpu.make_async_copy(w_two_ref, weights, load_weights)
    copy_normed_two = pltpu.make_async_copy(normed_two_ref, normed, load_normed)
    copy_normed_one = pltpu.make_async_copy(normed_one_ref, normed, load_normed)
    for copy in (copy_rows, copy_act_two, copy_w_three, copy_normed_two):
        copy.start()
    greet(everyone(spot))
    copy_rows.wait()

    def produce(t, slot):
        @pl.when(t < 16)
        def _():
            rhs = rows[t // 8, :, both(t % 8)]

            def tile(w):
                product = lax.dot_general(acts[:, pl.ds(pl.multiple_of(w * 512, 512), 512)], rhs, FIRST_DIMS,
                                          preferred_element_type=jnp.float32)
                slot[w] = product.reshape(2, 2, 2, BLOCK, CHUNK)

            looped(4, tile)

        @pl.when(t >= 16)
        def _():
            for k in range(4):
                product = jnp.dot(feat_ref[...], rows[2, :, both((t - 16) * 4 + k)], preferred_element_type=jnp.float32)
                slot[:, :, :, :, 16 * k:16 * k + 16, :] = product.reshape(4, 2, 2, 2, 16, CHUNK)

    def consume(j, block):
        @pl.when(j < 8)
        def _():
            out_three_ref[:, both(j)] = block

        @pl.when(jnp.logical_and(j >= 8, j < 16))
        def _():
            out_two_ref[:, both(j - 8)] = block

        @pl.when(j >= 16)
        def _():
            out_one_ref[j - 16] = block

    stream_step = stream_of(STREAM, spot, refs[:STREAM_REFS], produce, consume)

    def pull(layer, j):
        cols = both(j)
        gain, shift = aux_ref[1 - layer, 0:1, cols], aux_ref[1 - layer, 1:2, cols]
        weight = weights[cols, :]
        for view in range(2):
            span = slice(view * side, (view + 1) * side)
            grad = lax.dot_general(rows[layer, span, :], weight, (((1,), (1,)), ((), ())),
                                   preferred_element_type=jnp.float32)
            hat = normed[span, cols]
            grad = jnp.where(gain * hat + shift > 0, grad, 0.0)
            masked[span, cols] = grad
            part_sums[view:view + 1, cols] = jnp.sum(grad, axis=0, keepdims=True)
            part_sums[2 + view:3 + view, cols] = jnp.sum(grad * hat, axis=0, keepdims=True)

    def push(layer, j):
        cols = both(j)
        gain = aux_ref[1 - layer, 0:1, cols]
        for view in range(2):
            span = slice(view * side, (view + 1) * side)
            inv = inv_ref[1 - layer, view:view + 1, cols]
            sum_one = sums[layer, view:view + 1, cols] / count
            sum_two = sums[layer, 2 + view:3 + view, cols] / count
            grad = inv * (masked[span, cols] - (sum_one + normed[span, cols] * sum_two))
            rows[layer + 1, span, cols] = (gain * grad).astype(jnp.bfloat16)

    def descend_step(t):
        layer, phase = t // 8, t % 8

        def at(k):
            return pl.when(jnp.logical_and(t < 16, phase == k))

        def pulls(lo, hi):
            def body(j, carry):
                pull(layer, j)
                return carry
            lax.fori_loop(lo, hi, body, 0)

        def pushes(lo, hi):
            def body(j, carry):
                push(layer, j)
                return carry
            lax.fori_loop(lo, hi, body, 0)

        @at(1)
        def _():
            copy_w_three.wait()
            copy_normed_two.wait()

        @pl.when(jnp.logical_and(t < 16, jnp.logical_and(phase >= 1, phase <= 4)))
        def _():
            pulls(2 * phase - 2, 2 * phase)

        @at(4)
        def _():
            begin(layer)

        @pl.when(t == 4)
        def _():
            copy_w_two.start()

        @at(5)
        def _():
            cross(layer)

        @at(6)
        def _():
            finish(layer)
            pushes(0, 3)

        @at(7)
        def _():
            pushes(3, 8)

        @pl.when(t == 7)
        def _():
            copy_act_one.start()
            copy_normed_one.start()

    def step(t, carry):
        @pl.when(t == 0)
        def _():
            copy_act_two.wait()

        @pl.when(t == 8)
        def _():
            copy_act_one.wait()

        @pl.when(jnp.logical_and(t < 16, t % 8 == 6))
        def _():
            spread(t // 8)

        stream_step(t)
        descend_step(t)
        return carry

    lax.fori_loop(0, STREAM + 4, step, 0)
    sums_ref[...] = sums[...]


def descend(top, act_two, act_one, feat_t, w_three, w_two, normed_two, normed_one, aux, inv, collective_id):
    depth, features = top.shape
    dma, f32, bf16 = pltpu.SemaphoreType.DMA, jnp.float32, jnp.bfloat16
    away = pl.BlockSpec(memory_space=pltpu.HBM)
    return pl.pallas_call(
        descent_kernel,
        out_shape=(jax.ShapeDtypeStruct((BLOCK, features), f32), jax.ShapeDtypeStruct((BLOCK, features), f32),
                   jax.ShapeDtypeStruct((2, BLOCK, CHUNK), f32), jax.ShapeDtypeStruct((2, 4, features), f32)),
        in_specs=[away, away, away, VMEM, away, away, away, away, VMEM, VMEM], out_specs=(VMEM,) * 4,
        scratch_shapes=[pltpu.VMEM((3, depth, features), bf16), pltpu.VMEM((depth, features), bf16),
                        pltpu.VMEM((features, features), bf16), pltpu.VMEM((depth, features), f32),
                        pltpu.VMEM((depth, features), f32),
                        ] + [dma] * 4 + stream_scratch() + exchange_scratch(2, 4, features),
        compiler_params=params(collective_id),
        name="descend",
    )(top, act_two, act_one, feat_t, w_three, w_two, normed_two, normed_one, aux, inv)


def solution(mesh):
    shards = mesh.shape[AXIS]

    def local_step(h_a, h_b, w_one, w_two, w_three, gain_one, shift_one, gain_two, shift_two, lam_off):
        rows_dev = h_a.shape[0]
        features = w_two.shape[0]
        in_rows = h_a.shape[1] // shards

        def turned(view):
            blocks = jnp.pad(view.T.reshape(shards, in_rows, rows_dev), ((0, 0), (0, 16 - in_rows), (0, 0)))
            return blocks.reshape(shards * 16, rows_dev)

        feat_t = jnp.concatenate([turned(h_a), turned(h_b)], axis=1)
        aux = jnp.stack([jnp.stack([gain_one, shift_one]), jnp.stack([gain_two, shift_two])])
        hat_one, hat_two, hat_out, act_one, act_two, embed, inv = ascend(h_a, h_b, w_one, w_two, w_three, aux, 0)
        top, loss_total = correlate(embed, hat_out, inv, lam_off.reshape(1, 1), 1)
        out_three, out_two, out_one, sums = descend(top, act_two, act_one, feat_t, w_three, w_two, hat_two, hat_one, aux, inv, 2)
        grad_w_one = out_one.reshape(2, 4, 16, CHUNK).transpose(2, 0, 1, 3).reshape(16, features)[:in_rows]
        return (loss_total.reshape(()), grad_w_one, out_two, out_three,
                sums[1, 2] + sums[1, 3], sums[1, 0] + sums[1, 1], sums[0, 2] + sums[0, 3], sums[0, 0] + sums[0, 1])

    row_spec = P(AXIS, None)
    whole_mat = P(None, None)
    whole_vec = P(None)
    return jax.shard_map(
        local_step, mesh=mesh,
        in_specs=(row_spec, row_spec, whole_mat, whole_mat, whole_mat,
                  whole_vec, whole_vec, whole_vec, whole_vec, P()),
        out_specs=(P(), row_spec, row_spec, row_spec, whole_vec, whole_vec, whole_vec, whole_vec),
        check_vma=False)
```
